256 devices in a mesh: dp: 64 (over z, y, core), pp: 4 (over x).
Axes of the slice: x: 4, y: 4, z: 8, core: 2. Of those that a mesh axis runs over, the one named last changes fastest.
Arguments:
- x_in: bfloat16 [2, 64, 197, 768], P(None, 'dp')
- grad_out: bfloat16 [2, 64, 197, 768], P(None, 'dp')
- vectors: bfloat16 [4, 9, 768], P('pp')
- w_qkv: bfloat16 [4, 768, 2304], P('pp')
- w_proj: bfloat16 [4, 12, 64, 768], P('pp')
- w_fc1: bfloat16 [4, 768, 3072], P('pp')
- b_fc1: bfloat16 [4, 3072], P('pp')
- w_fc2: bfloat16 [4, 3072, 768], P('pp')
Outputs:
- output 1: bfloat16 [4, 2, 64, 197, 768], P('pp', None, 'dp')
- output 2: bfloat16 [4, 2, 64, 197, 768], P('pp', None, 'dp')
- output 3: float32 [4, 9, 768], P('pp')
- output 4: float32 [4, 768, 2304], P('pp')
- output 5: float32 [4, 12, 64, 768], P('pp')
- output 6: float32 [4, 768, 3072], P('pp')
- output 7: float32 [4, 3072], P('pp')
- output 8: float32 [4, 3072, 768], P('pp')
All inputs are finite; a program needn't handle non-finite values.
Results may differ from the reference program's by a relative error of at most 0.02.
Values are sent between devices in bfloat16 or wider.
A program may use at most 768 MiB of HBM per device.

```python
import math
import jax
import jax.numpy as jnp
from jax import lax

MICRO_BATCHES = 2
GLOBAL_BATCH = 64
SEQ_TOKENS = 197
MODEL_WIDTH = 768
NUM_HEADS = 12
MLP_WIDTH = 3072
STAGES = 4
HEAD_DIM = MODEL_WIDTH // NUM_HEADS


def to_bf16(tensor):
    return tensor.astype(jnp.bfloat16).astype(jnp.float32)


def layer_norm(feat_in, ln_gain, ln_shift):
    mean_val = jnp.mean(feat_in, axis=-1, keepdims=True)
    centered = feat_in - mean_val
    var_val = jnp.mean(centered * centered, axis=-1, keepdims=True)
    return centered * lax.rsqrt(var_val + 1e-5) * ln_gain + ln_shift


def layer_forward(h_in, layer_params):
    vectors, w_qkv, w_proj, w_fc1, b_fc1, w_fc2 = layer_params
    attn_scale = 1.0 / math.sqrt(HEAD_DIM)
    in_f32 = h_in.astype(jnp.float32)
    ln1_out = to_bf16(layer_norm(in_f32, vectors[0], vectors[1]))
    qkv_act = to_bf16(jnp.dot(ln1_out, w_qkv, preferred_element_type=jnp.float32) + vectors[2:5].reshape(3 * MODEL_WIDTH))
    qkv_heads = qkv_act.reshape(SEQ_TOKENS, 3, NUM_HEADS, HEAD_DIM)
    scores = to_bf16(jnp.einsum('qhd,khd->hqk', qkv_heads[:, 0], qkv_heads[:, 1]) * attn_scale)
    attn_probs = to_bf16(jax.nn.softmax(scores, axis=-1))
    attn_out = to_bf16(jnp.einsum('hqk,khd->qhd', attn_probs, qkv_heads[:, 2])).reshape(SEQ_TOKENS, MODEL_WIDTH)
    resid_mid = to_bf16(in_f32 + jnp.dot(attn_out, w_proj.reshape(MODEL_WIDTH, MODEL_WIDTH), preferred_element_type=jnp.float32) + vectors[5])
    ln2_out = to_bf16(layer_norm(resid_mid, vectors[6], vectors[7]))
    pre_act = to_bf16(jnp.dot(ln2_out, w_fc1, preferred_element_type=jnp.float32) + b_fc1)
    mlp_act = to_bf16(jax.nn.gelu(pre_act, approximate=False))
    return (resid_mid + jnp.dot(mlp_act, w_fc2, preferred_element_type=jnp.float32) + vectors[8]).astype(jnp.bfloat16)


def setup_inputs(seed: int = 0) -> dict:
    rand_keys = jax.random.split(jax.random.key(seed), 8)
    grad_scale = 1.0 / math.sqrt(math.sqrt(MICRO_BATCHES * GLOBAL_BATCH * SEQ_TOKENS))
    act_shape = (MICRO_BATCHES, GLOBAL_BATCH, SEQ_TOKENS, MODEL_WIDTH)
    x_in = jax.random.normal(rand_keys[0], act_shape, jnp.float32).astype(jnp.bfloat16)
    grad_out = (jax.random.normal(rand_keys[1], act_shape, jnp.float32) * grad_scale).astype(jnp.bfloat16)
    gain_rows = jnp.array([1.0, 0.0, 0.0, 0.0, 0.0, 0.0, 1.0, 0.0, 0.0], jnp.float32)[None, :, None]
    vectors = (gain_rows + 0.2 * jax.random.normal(rand_keys[2], (STAGES, 9, MODEL_WIDTH), jnp.float32)).astype(jnp.bfloat16)
    w_qkv = (jax.random.normal(rand_keys[3], (STAGES, MODEL_WIDTH, 3 * MODEL_WIDTH), jnp.float32) / math.sqrt(MODEL_WIDTH)).astype(jnp.bfloat16)
    w_proj = (jax.random.normal(rand_keys[4], (STAGES, NUM_HEADS, HEAD_DIM, MODEL_WIDTH), jnp.float32) / math.sqrt(MODEL_WIDTH)).astype(jnp.bfloat16)
    w_fc1 = (jax.random.normal(rand_keys[5], (STAGES, MODEL_WIDTH, MLP_WIDTH), jnp.float32) / math.sqrt(MODEL_WIDTH)).astype(jnp.bfloat16)
    b_fc1 = (0.5 * jax.random.normal(rand_keys[6], (STAGES, MLP_WIDTH), jnp.float32)).astype(jnp.bfloat16)
    w_fc2 = (jax.random.normal(rand_keys[7], (STAGES, MLP_WIDTH, MODEL_WIDTH), jnp.float32) / math.sqrt(MLP_WIDTH)).astype(jnp.bfloat16)
    return {'x_in': x_in, 'grad_out': grad_out, 'vectors': vectors, 'w_qkv': w_qkv, 'w_proj': w_proj, 'w_fc1': w_fc1, 'b_fc1': b_fc1, 'w_fc2': w_fc2}


def reference(x_in, grad_out, vectors, w_qkv, w_proj, w_fc1, b_fc1, w_fc2):
    params = (vectors.astype(jnp.float32), w_qkv.astype(jnp.float32), w_proj.astype(jnp.float32), w_fc1.astype(jnp.float32), b_fc1.astype(jnp.float32), w_fc2.astype(jnp.float32))
    sample_count = MICRO_BATCHES * GLOBAL_BATCH
    samples = x_in.reshape(sample_count, SEQ_TOKENS, MODEL_WIDTH)
    sample_cts = grad_out.reshape(sample_count, SEQ_TOKENS, MODEL_WIDTH)

    def fwd_step(h_cur, layer_params):
        h_next = layer_forward(h_cur, layer_params)
        return h_next, (h_cur, h_next)

    def bwd_step(ct_cur, step_inputs):
        h_cur, layer_params = step_inputs
        _, pull_back = jax.vjp(layer_forward, h_cur, layer_params)
        ct_in, ct_params = pull_back(ct_cur)
        return ct_in, (ct_in, ct_params)

    def per_sample(grad_acc, sample_pair):
        sample_in, sample_ct = sample_pair
        _, (layer_ins, layer_outs) = lax.scan(fwd_step, sample_in, params)
        _, (layer_cts, param_cts) = lax.scan(bwd_step, sample_ct, (layer_ins, params), reverse=True)
        return jax.tree.map(jnp.add, grad_acc, param_cts), (layer_outs, layer_cts)

    zero_acc = jax.tree.map(jnp.zeros_like, params)
    grads_w, (outs_all, cts_all) = lax.scan(per_sample, zero_acc, (samples, sample_cts))
    full_shape = (MICRO_BATCHES, GLOBAL_BATCH, STAGES, SEQ_TOKENS, MODEL_WIDTH)
    stage_out = outs_all.reshape(full_shape).transpose(2, 0, 1, 3, 4)
    stage_grad = cts_all.reshape(full_shape).transpose(2, 0, 1, 3, 4)
    return (stage_out, stage_grad, grads_w[0], grads_w[1], grads_w[2], grads_w[3], grads_w[4], grads_w[5])
```

```python
import functools
import heapq
import math
import jax
import jax.numpy as jnp
from jax import lax
from jax.experimental import pallas as pl
from jax.experimental.pallas import tpu as pltpu
from jax.sharding import PartitionSpec as P

MESH = pl.DeviceIdType.MESH
F32 = jnp.float32
BF16 = jnp.bfloat16
TOK = 208
KEYS = 256
LANES = 128
SHIFT = 6200
PAIRS = 3


def dot_nn(a, b):
    return lax.dot_general(a, b, (((1,), (0,)), ((), ())), preferred_element_type=F32)


def dot_nt(a, b):
    return lax.dot_general(a, b, (((1,), (1,)), ((), ())), preferred_element_type=F32)


def dot_tn(a, b):
    return lax.dot_general(a, b, (((0,), (0,)), ((), ())), preferred_element_type=F32)


def rounded(x):
    return x.astype(BF16).astype(F32)


def aligned(start, size):
    return pl.ds(pl.multiple_of(start, LANES), size)


def pipeline_kernel(cfg, x_in, go_in, vec_ref, bf1_ref, wqkv_in, wproj_in, w1_in, w2_in,
                    so_out, sg_out, xa1, xa2, xo, xf, dqkv_out, dz_out, dr_out, gy_out, vec_out,
                    wqkv, wproj, w1, w2, wqkv_t, wproj_t, w1_t, w2_t, xt, hbuf, gbuf, obuf, gibuf, a1, qkv, att, res, a2, zact, fact, prob, stats,
                    dz, dres, datt, dqkv, vsum,
                    w_sem, in_sem, send_sem, recv_sem, loc_sem, psend_sem, precv_sem, vec_sem):
    seq, stages, n_micro = cfg
    width = wproj.shape[0]
    mlp = w1.shape[1]
    heads = width // 64
    half_qkv, half_mlp, half_w = 3 * width // 2, mlp // 2, width // 2
    dp = lax.axis_index('dp')
    stage = lax.axis_index('pp')
    core = lax.rem(dp, 2)
    mate = dp + 1 - 2 * core
    other = 1 - core
    last = stages - 1
    nxt = lax.rem(stage + 1, stages)
    prv = lax.rem(stage + stages - 1, stages)

    loads = [pltpu.make_async_copy(src, dst, w_sem.at[i])
             for i, (src, dst) in enumerate(((wqkv_in, wqkv), (wproj_in, wproj), (w1_in, w1), (w2_in, w2)))]

    def x_load(m):
        return pltpu.make_async_copy(x_in.at[m], hbuf.at[m], in_sem.at[m])

    def g_load(m):
        return pltpu.make_async_copy(go_in.at[m], gbuf.at[m], in_sem.at[n_micro + m])

    @pl.when(stage == 0)
    def _():
        for m in range(n_micro):
            x_load(m).start()
    for ld in loads:
        ld.start()

    @pl.when(stage == last)
    def _():
        for m in range(n_micro):
            g_load(m).start()

    @pl.when((stage == 0) & (core == 1))
    def _():
        pl.delay(SHIFT)

    barrier = pltpu.get_barrier_semaphore()
    pl.semaphore_signal(barrier, inc=1, device_id={'pp': nxt}, device_id_type=MESH)
    pl.semaphore_signal(barrier, inc=1, device_id={'pp': prv}, device_id_type=MESH)
    pl.semaphore_signal(barrier, inc=1, device_id={'dp': mate}, device_id_type=MESH)

    qkv[:, TOK:, :] = jnp.zeros((n_micro, KEYS - TOK, 3 * width), BF16)
    vsum[...] = jnp.zeros(vsum.shape, F32)
    pl.semaphore_wait(barrier, 3)

    def fwd_copy(m):
        return pltpu.make_async_remote_copy(obuf.at[m], hbuf.at[m], send_sem.at[m], recv_sem.at[m],
                                            device_id={'pp': nxt}, device_id_type=MESH)

    def bwd_copy(m):
        return pltpu.make_async_remote_copy(gibuf.at[m], gbuf.at[m], send_sem.at[n_micro + m], recv_sem.at[n_micro + m],
                                            device_id={'pp': prv}, device_id_type=MESH)

    def local(src, dst, m, i):
        return pltpu.make_async_copy(src, dst, loc_sem.at[m, i])

    def to_mate(src, dst, m, i):
        return pltpu.make_async_remote_copy(src, dst, psend_sem.at[m, i], precv_sem.at[m, i],
                                            device_id={'dp': mate}, device_id_type=MESH)

    def fwd_exports(m):
        own, fore = [pl.ds(pl.multiple_of(3 * width + c * half_mlp, LANES), half_mlp) for c in (core, other)]
        first, second, third = [slice(i * width, (i + 1) * width) for i in range(3)]
        loc = [local(xt.at[m, first], xa1.at[m], m, 0), local(xt.at[m, second], xa2.at[m], m, 1),
               local(xt.at[m, third], xo.at[m], m, 2), local(xt.at[m, own], xf.at[m], m, 3)]
        far = [to_mate(xt.at[m, first], xa1.at[n_micro + m], m, 0), to_mate(xt.at[m, second], xa2.at[n_micro + m], m, 1),
               to_mate(xt.at[m, third], xo.at[n_micro + m], m, 2), to_mate(xt.at[m, fore], xf.at[n_micro + m], m, 3)]
        return loc, far

    def out_copy(m):
        return local(obuf.at[m], so_out.at[m], m, 4)

    def bwd_exports(m):
        own, fore = [[aligned(c * h, h) for h in (half_mlp, half_w, half_qkv)] for c in (core, other)]
        loc = [local(gbuf.at[m], gy_out.at[m], m, 5), local(dz.at[m, :, own[0]], dz_out.at[m], m, 6),
               local(dres.at[m, :, own[1]], dr_out.at[m], m, 7), local(dqkv.at[m, :, own[2]], dqkv_out.at[m], m, 8),
               local(gibuf.at[m], sg_out.at[m], m, 9)]
        far = [to_mate(gbuf.at[m], gy_out.at[n_micro + m], m, 4), to_mate(dz.at[m, :, fore[0]], dz_out.at[n_micro + m], m, 5),
               to_mate(dres.at[m, :, fore[1]], dr_out.at[n_micro + m], m, 6),
               to_mate(dqkv.at[m, :, fore[2]], dqkv_out.at[n_micro + m], m, 7)]
        return loc, far

    def row(i):
        return vec_ref[i:i + 1, :].astype(F32)

    def norm(m, src, idx):
        mean = jnp.sum(src, axis=-1, keepdims=True) * (1.0 / width)
        cen = src - mean
        var = jnp.sum(cen * cen, axis=-1, keepdims=True) * (1.0 / width)
        rs = lax.rsqrt(var + 1e-5)
        stats[m, 2 * idx] = mean
        stats[m, 2 * idx + 1] = rs
        return cen * rs

    def add_vec(i, val):
        for t in range(val.shape[1] // LANES):
            vsum[i + t:i + t + 1, :] = vsum[i + t:i + t + 1, :] + val[:, LANES * t:LANES * (t + 1)]

    lane = lax.broadcasted_iota(jnp.int32, (1, LANES), 1)
    head_mask = [(lane < 64).astype(F32).astype(BF16), (lane >= 64).astype(F32).astype(BF16)]
    key_ok = lax.broadcasted_iota(jnp.int32, (TOK, KEYS), 1) < seq
    scale = 1.0 / math.sqrt(64)
    n_tile = mlp // width

    def flip_weights():
        def blocks(n, src, dst, by_row):
            def body(i, c):
                at = pl.ds(pl.multiple_of(i * KEYS, LANES), KEYS)
                if by_row:
                    dst[:, at] = src[at, :].T
                else:
                    dst[at, :] = src[:, at].T
                return c
            lax.fori_loop(0, n, body, 0)
        blocks(mlp // KEYS, w2, w2_t, True)
        blocks(mlp // KEYS, w1, w1_t, False)
        blocks(width // KEYS, wproj, wproj_t, False)
        blocks(3 * width // KEYS, wqkv, wqkv_t, False)

    def flip_acts(m, carry):
        fill = jnp.zeros((KEYS - TOK, width), BF16)
        for i, src in enumerate((a1, a2, att)):
            xt[m, i * width:(i + 1) * width, :] = jnp.concatenate([src[m], fill], axis=0).T

        def body(j, c):
            rows = pl.ds(pl.multiple_of((3 + j) * width, LANES), width)
            xt[m, rows, :] = jnp.concatenate([fact[m, :, aligned(j * width, width)], fill], axis=0).T
            return c
        lax.fori_loop(0, n_tile, body, 0)
        loc, far = fwd_exports(m)
        for c in loc + far:
            c.start()
        return carry

    def forward(m, carry):
        @pl.when(stage == 0)
        def _():
            x_load(m).wait()

        @pl.when(stage > 0)
        def _():
            fwd_copy(m).wait_recv()

        h = hbuf[m].astype(F32)
        a1[m] = (norm(m, h, 0) * row(0) + row(1)).astype(BF16)

        @pl.when((m == 0) & (stage == 0))
        def _():
            loads[0].wait()
        for j in range(3):
            cols = slice(j * width, (j + 1) * width)
            qkv[m, :TOK, cols] = (dot_nn(a1[m], wqkv[:, cols]) + row(2 + j)).astype(BF16)

        def attend(p):
            q2 = qkv[m, :TOK, aligned(p * LANES, LANES)]
            k2 = qkv[m, :, aligned(width + p * LANES, LANES)]
            v2 = qkv[m, :, aligned(2 * width + p * LANES, LANES)]
            out = None
            for e in range(2):
                s = rounded(dot_nt(q2 * head_mask[e], k2) * scale)
                s = jnp.where(key_ok, s, -1e30)
                ex = jnp.exp(s - jnp.max(s, axis=-1, keepdims=True))
                pr = ex * (1.0 / jnp.sum(ex, axis=-1, keepdims=True))
                prob[m, 2 * p + e] = pr
                o = dot_nn(pr.astype(BF16), v2 * head_mask[e])
                out = o if out is None else out + o
            att[m, :, aligned(p * LANES, LANES)] = out.astype(BF16)

        def attend_some(i, c):
            for j in range(PAIRS):
                attend(PAIRS * i + j)
            return c
        lax.fori_loop(0, heads // 2 // PAIRS, attend_some, 0)

        @pl.when((m == 0) & (stage == 0))
        def _():
            loads[1].wait()
        r = (hbuf[m].astype(F32) + dot_nn(att[m], wproj[...]) + row(5)).astype(BF16)
        res[m] = r
        a2[m] = (norm(m, r.astype(F32), 1) * row(6) + row(7)).astype(BF16)

        @pl.when((m == 0) & (stage == 0))
        def _():
            loads[2].wait()

        def expand(j, c):
            cols = aligned(j * width, width)
            z = (dot_nn(a2[m], w1[:, cols]) + bf1_ref[:, cols].astype(F32)).astype(BF16)
            zact[m, :, cols] = z
            z = z.astype(F32)
            fact[m, :, cols] = (z * (0.5 + 0.5 * lax.erf(z * math.sqrt(0.5)))).astype(BF16)
            return c
        lax.fori_loop(0, n_tile, expand, 0)

        @pl.when((m == 0) & (stage == 0))
        def _():
            loads[3].wait()
        obuf[m] = (res[m].astype(F32) + dot_nn(fact[m], w2[...]) + row(8)).astype(BF16)

        @pl.when(stage < last)
        def _():
            fwd_copy(m).start()
        out_copy(m).start()
        return carry

    def norm_back(m, src, idx, g, gain, shift_row, skip):
        xhat = (src - stats[m, 2 * idx]) * stats[m, 2 * idx + 1]
        add_vec(shift_row, jnp.sum(g, axis=0, keepdims=True))
        gx = g * xhat
        add_vec(shift_row - width // LANES, jnp.sum(gx, axis=0, keepdims=True))
        m1 = jnp.sum(g * gain, axis=-1, keepdims=True) * (1.0 / width)
        m2 = jnp.sum(gx * gain, axis=-1, keepdims=True) * (1.0 / width)
        return (skip + stats[m, 2 * idx + 1] * (g * gain - m1 - xhat * m2)).astype(BF16)

    vr = width // LANES

    def backward(m, carry):
        @pl.when(stage == last)
        def _():
            g_load(m).wait()

        @pl.when(stage < last)
        def _():
            bwd_copy(m).wait_recv()

        def contract(j, c):
            cols = aligned(j * width, width)
            ga = rounded(dot_nn(gbuf[m], w2_t[:, cols]))
            z = zact[m, :, cols].astype(F32)
            cdf = 0.5 + 0.5 * lax.erf(z * math.sqrt(0.5))
            pdf = jnp.exp(z * z * -0.5) * (1.0 / math.sqrt(2.0 * math.pi))
            dz[m, :, cols] = (ga * (cdf + z * pdf)).astype(BF16)
            return c
        lax.fori_loop(0, n_tile, contract, 0)
        g2 = rounded(dot_nn(dz[m], w1_t[...]))
        dr = norm_back(m, res[m].astype(F32), 1, g2, row(6), 7 * vr, gbuf[m].astype(F32))
        dres[m] = dr
        datt[...] = dot_nn(dr, wproj_t[...]).astype(BF16)

        def attend_back(p):
            q2 = qkv[m, :TOK, aligned(p * LANES, LANES)]
            k2 = qkv[m, :, aligned(width + p * LANES, LANES)]
            v2 = qkv[m, :, aligned(2 * width + p * LANES, LANES)]
            do2 = datt[:, aligned(p * LANES, LANES)]
            dq = dk = dv = None
            for e in range(2):
                pr = prob[m, 2 * p + e]
                qe, ke, de = q2 * head_mask[e], k2 * head_mask[e], do2 * head_mask[e]
                dp_ = rounded(dot_nt(de, v2))
                t = jnp.sum(pr * dp_, axis=-1, keepdims=True)
                ds = (pr * (dp_ - t)).astype(BF16)
                parts = dot_nn(ds, ke), dot_tn(ds, qe), dot_tn(pr.astype(BF16), de)
                dq, dk, dv = parts if dq is None else (dq + parts[0], dk + parts[1], dv + parts[2])
            dqkv[m, :, aligned(p * LANES, LANES)] = (dq * scale).astype(BF16)
            dqkv[m, :, aligned(width + p * LANES, LANES)] = (dk[:TOK] * scale).astype(BF16)
            dqkv[m, :, aligned(2 * width + p * LANES, LANES)] = dv[:TOK].astype(BF16)

        def attend_back_some(i, c):
            for j in range(PAIRS):
                attend_back(PAIRS * i + j)
            return c
        lax.fori_loop(0, heads // 2 // PAIRS, attend_back_some, 0)
        g1 = rounded(dot_nn(dqkv[m], wqkv_t[...]))
        gibuf[m] = norm_back(m, hbuf[m].astype(F32), 0, g1, row(0), vr, dres[m].astype(F32))

        @pl.when(stage > 0)
        def _():
            bwd_copy(m).start()
        loc, far = bwd_exports(m)
        for c in loc + far:
            c.start()
        return carry

    @pl.when(stage > 0)
    def _():
        for ld in loads:
            ld.wait()
        flip_weights()
    lax.fori_loop(0, n_micro, forward, 0)

    @pl.when(stage == 0)
    def _():
        flip_weights()

    @pl.when(stage < last)
    def _():
        lax.fori_loop(0, n_micro, flip_acts, 0)
    lax.fori_loop(0, n_micro, backward, 0)

    @pl.when(stage == last)
    def _():
        lax.fori_loop(0, n_micro, flip_acts, 0)

    def sums(m, carry):
        for j in range(3):
            add_vec((2 + j) * vr, jnp.sum(dqkv[m, :, j * width:(j + 1) * width].astype(F32), axis=0, keepdims=True))
        add_vec(5 * vr, jnp.sum(dres[m].astype(F32), axis=0, keepdims=True))
        add_vec(8 * vr, jnp.sum(gbuf[m].astype(F32), axis=0, keepdims=True))
        for j in range(n_tile):
            add_vec(9 * vr + j * vr, jnp.sum(dz[m, :, j * width:(j + 1) * width].astype(F32), axis=0, keepdims=True))
        return carry
    lax.fori_loop(0, n_micro, sums, 0)

    vec_loc = pltpu.make_async_copy(vsum, vec_out.at[0], vec_sem.at[0])
    vec_far = pltpu.make_async_remote_copy(vsum, vec_out.at[1], vec_sem.at[1], vec_sem.at[2],
                                           device_id={'dp': mate}, device_id_type=MESH)
    vec_loc.start()
    vec_far.start()
    for m in range(n_micro):
        @pl.when(stage < last)
        def _():
            fwd_copy(m).wait_send()

        @pl.when(stage > 0)
        def _():
            bwd_copy(m).wait_send()
        out_copy(m).wait()
        for loc, far in (fwd_exports(m), bwd_exports(m)):
            for c in loc:
                c.wait()
            for c in far:
                c.wait_send()
                c.wait_recv()
    vec_loc.wait()
    vec_far.wait_send()
    vec_far.wait_recv()


FIRST_Y = {'fc1': True, 'qkv': True, 'fc2': False, 'proj': False, 'vec': True}
ROWS = {'fc1': 768, 'qkv': 768, 'fc2': 1536, 'proj': 768, 'vec': 256}
PLUS = {'fc1': 6, 'qkv': 5, 'fc2': 3, 'proj': 2}
MINUS = {'fc1': 6, 'qkv': 4, 'fc2': 3, 'proj': 1}
WIDEST = {'fc1': 2, 'qkv': 2, 'fc2': 1, 'proj': 1}


def make_pieces():
    pieces = []
    for name in ('fc1', 'qkv', 'fc2', 'proj'):
        col = 0
        for way, tiles in ((1, PLUS[name]), (-1, MINUS[name])):
            k = -(-tiles // WIDEST[name])
            for i in range(k):
                t = tiles // k + (1 if i < tiles % k else 0)
                pieces.append((name, way, col * LANES, t * LANES))
                col += t
    return pieces + [('vec', 1, 0, LANES)]


def make_order(pieces, ny, nz, rate=51.3e3, lat=2.79, lat_y=0.3, first=5.0, ready=15.0, step=0.0736):
    heap, order, waiting, free, count = [], [], {}, {}, [0]

    def on_y(i, ph):
        return FIRST_Y[pieces[i][0]] == (ph == 1)

    def ring(i, ph):
        return ny if on_y(i, ph) else nz

    def nbytes(i, ph):
        rows = ROWS[pieces[i][0]] // ring(i, 1)
        return (rows if ph == 1 else rows // ring(i, 2)) * pieces[i][3] * 4

    def push(t, item):
        count[0] += 1
        heapq.heappush(heap, (t, count[0], item))

    def dispatch(t, key):
        queue = waiting.get(key)
        if queue and free.get(key, 0.0) <= t + 1e-9:
            typ, i, ph, k = heapq.heappop(queue)[-1]
            w = nbytes(i, ph) / rate
            free[key] = t + w
            order.append(('send', typ, i, ph, k))
            push(t + w, ('free', key))
            push(t + w + lat + (lat_y if key[0] else 0.0), ('land', (typ, i, ph, k)))

    def enqueue(t, typ, i, ph, k):
        way = pieces[i][1] * (1 if typ == 'rs' else -1)
        key = (on_y(i, ph), way)
        count[0] += 1
        heapq.heappush(waiting.setdefault(key, []), ((ph == 1 and typ == 'ag', ph == 1, -k if typ == 'rs' else 0, i), count[0], (typ, i, ph, k)))
        dispatch(t, key)

    for i in range(len(pieces)):
        push(first, ('start', i))
    seq = ready
    while heap:
        t, _, item = heapq.heappop(heap)
        if item[0] == 'free':
            dispatch(t, item[1])
        elif item[0] == 'start':
            enqueue(t, 'rs', item[1], 1, 0)
        elif item[0] == 'land':
            seq = max(seq, t) + step
            push(seq, ('done', item[1]))
        else:
            typ, i, ph, k = item[1]
            order.append(('recv', typ, i, ph, k))
            if k < ring(i, ph) - 2:
                enqueue(t, typ, i, ph, k + 1)
            elif typ == 'rs':
                enqueue(t, 'rs' if ph == 1 else 'ag', i, 2, 0)
            elif ph == 2:
                enqueue(t, 'ag', i, 1, 0)
    return order


def grad_kernel(cfg, *refs):
    ny, nz, n_img, pieces, order = cfg
    n_p = len(pieces)
    it = iter(refs)
    take = lambda n: [next(it) for _ in range(n)]
    x_in = dict(zip(('fc1', 'fc2', 'qkv', 'proj'), take(4)))
    y_in = dict(zip(('fc1', 'fc2', 'qkv', 'proj'), take(4)))
    (vec_in,) = take(1)
    out = dict(zip(('fc1', 'fc2', 'qkv', 'proj', 'vec'), take(5)))
    x_t = dict(zip(('fc1', 'fc2', 'qkv', 'proj'), take(4)))
    y_v = dict(zip(('fc1', 'fc2', 'qkv', 'proj'), take(4)))
    (vec_v,) = take(1)
    acc = dict(zip(('fc1', 'fc2', 'qkv', 'proj', 'vec'), take(5)))
    slot1, slot2 = take(n_p), take(n_p)
    ld_sem, send_sem, recv_sem, out_sem, mate_send, mate_recv = take(6)

    dp = lax.axis_index('dp')
    core = lax.rem(dp, 2)
    mate = dp + 1 - 2 * core
    py = lax.rem(lax.div(dp, 2), ny)
    pz = lax.div(dp, 2 * ny)

    def at(y, z):
        return (z * ny + y) * 2 + core

    def turn(pos, by, n):
        return lax.rem(pos + by % n, n)

    nbr = {(True, 1): at(turn(py, 1, ny), pz), (True, -1): at(turn(py, -1, ny), pz),
           (False, 1): at(py, turn(pz, 1, nz)), (False, -1): at(py, turn(pz, -1, nz))}

    names = ('fc1', 'fc2', 'qkv', 'proj')
    loads = []
    for j, name in enumerate(names):
        for s in range(n_img):
            loads.append((name, pltpu.make_async_copy(x_in[name].at[s], x_t[name].at[s], ld_sem.at[j, 0, s])))
            loads.append((name, pltpu.make_async_copy(y_in[name].at[s], y_v[name].at[s, 0:TOK, :], ld_sem.at[j, 1, s])))
    vec_load = pltpu.make_async_copy(vec_in, vec_v, ld_sem.at[4, 0, 0])
    for _, ld in loads:
        ld.start()
    vec_load.start()

    barrier = pltpu.get_barrier_semaphore()
    for dev in list(nbr.values()) + [mate]:
        pl.semaphore_signal(barrier, inc=1, device_id={'dp': dev}, device_id_type=MESH)

    for name in names:
        y_v[name][:, TOK:, :] = jnp.zeros((n_img, KEYS - TOK, y_v[name].shape[2]), BF16)
    pl.semaphore_wait(barrier, 5)

    def ring(i, ph):
        return ny if FIRST_Y[pieces[i][0]] == (ph == 1) else nz

    def place(i, ph):
        return py if FIRST_Y[pieces[i][0]] == (ph == 1) else pz

    def rows1(i, by):
        size = ROWS[pieces[i][0]] // ring(i, 1)
        return pl.ds(pl.multiple_of(turn(place(i, 1), by, ring(i, 1)) * size, 8), size)

    def rows2(i, by):
        big = ROWS[pieces[i][0]] // ring(i, 1)
        size = big // ring(i, 2)
        return pl.ds(pl.multiple_of(place(i, 1) * big + turn(place(i, 2), by, ring(i, 2)) * size, 8), size)

    def view(i, ph, by):
        name, _, col, cols = pieces[i]
        rows = rows1(i, by) if ph == 1 else rows2(i, by)
        return acc[name].at[rows, col:col + cols]

    steps = {}
    for _, typ, i, ph, k in order:
        steps.setdefault((typ, i, ph, k), len(steps))

    def landing(i, ph, k):
        n = ring(i, ph)
        return n - 3 - k if k <= n - 3 else n - 1

    def sent(group, i):
        slots = ((slot1, slot2)[group % 2])[i]
        part = slots.at[0:slots.shape[0] - 1]
        pltpu.make_async_copy(part, part, send_sem.at[group * n_p + i]).wait()

    def copy(typ, i, ph, k):
        way = pieces[i][1] * (1 if typ == 'rs' else -1)
        group = ((0 if typ == 'rs' else 2) + ph - 1) * n_p + i
        slots = (slot1 if ph == 1 else slot2)[i]
        if typ == 'rs':
            src, dst = view(i, ph, -way * (1 + k)), slots.at[k]
        else:
            src = slots.at[landing(i, ph, k - 1)] if k else view(i, ph, 0)
            dst = slots.at[landing(i, ph, k)]
        return pltpu.make_async_remote_copy(src, dst, send_sem.at[group], recv_sem.at[steps[typ, i, ph, k]],
                                            device_id={'dp': nbr[FIRST_Y[pieces[i][0]] == (ph == 1), way]}, device_id_type=MESH)

    def home(i, rows):
        name, _, col, cols = pieces[i]
        if name == 'vec':
            return out[name].at[rows, :]
        if name == 'fc2':
            return out[name].at[pl.ds(pl.multiple_of(core * ROWS[name] + rows.start, 8), rows.size), col:col + cols]
        half = (PLUS[name] + MINUS[name]) * LANES
        return out[name].at[rows, aligned(core * half + col, cols)]

    def deliver(i, src, by):
        name = pieces[i][0]
        dst = home(i, rows1(i, by))
        pltpu.make_async_copy(src, dst, out_sem.at[i]).start()
        if name != 'vec':
            pltpu.make_async_remote_copy(src, dst, mate_send.at[i], mate_recv.at[i],
                                         device_id={'dp': mate}, device_id_type=MESH).start()

    def multiply(k, c, name):
        i = next(j for j in range(n_p) if pieces[j][0] == name)
        size = ROWS[name] // ring(i, 1)
        split = PLUS[name] * LANES
        for way, cols in ((1, slice(0, split)), (-1, slice(split, split + MINUS[name] * LANES))):
            idx = lax.rem(place(i, 1) + (2 * ring(i, 1) - way) - way * k, ring(i, 1))
            rows = pl.ds(pl.multiple_of(idx * size, 8), size)
            acc[name][rows, cols] = sum(dot_nn(x_t[name][s, rows, :], y_v[name][s, :, cols]) for s in range(n_img))
        return c

    n_first = next(j for j, o in enumerate(order) if o[0] == 'recv')
    begin, todo = order[:n_first], order[n_first:]
    for name in ('vec',) + names:
        if name == 'vec':
            vec_load.wait()
            acc['vec'][...] = vec_v[0] + vec_v[1]
        else:
            for nm, ld in loads:
                if nm == name:
                    ld.wait()
            multiply(0, 0, name)
        for o in begin:
            if pieces[o[2]][0] == name:
                copy(*o[1:]).start()
    for name in names:
        i = next(j for j in range(n_p) if pieces[j][0] == name)
        lax.fori_loop(1, ring(i, 1), functools.partial(multiply, name=name), 0)

    for what, typ, i, ph, k in todo:
        if what == 'send':
            copy(typ, i, ph, k).start()
            continue
        copy(typ, i, ph, k).wait_recv()
        way = pieces[i][1] * (1 if typ == 'rs' else -1)
        if typ == 'rs':
            dst = view(i, ph, -way * (2 + k))
            dst[...] = dst[...] + (slot1 if ph == 1 else slot2)[i][k]
        elif ph == 1:
            deliver(i, slot1[i].at[landing(i, 1, k)], -way * (1 + k))
        elif k == ring(i, 2) - 2:
            sent(1, i)
            for j in range(ring(i, 2) - 1):
                dst = view(i, 2, -way * (1 + j))
                dst[...] = slot2[i][landing(i, 2, j)]
            deliver(i, view(i, 1, 0), 0)

    for i in range(n_p):
        name, _, col, cols = pieces[i]
        for group in (0, 2, 3):
            sent(group, i)
        whole = acc[name].at[:, col:col + cols]
        pltpu.make_async_copy(whole, whole, out_sem.at[i]).wait()
        if name != 'vec':
            pltpu.make_async_copy(whole, whole, mate_send.at[i]).wait()
            pltpu.make_async_copy(whole, whole, mate_recv.at[i]).wait()


def solution(mesh):
    stages = mesh.shape['pp']
    n_dp = mesh.shape['dp']
    ny = 4 if n_dp == 64 else 2
    nz = n_dp // (2 * ny)
    act_spec = P(None, 'dp')
    stage_spec = P('pp')
    out_act_spec = P('pp', None, 'dp')
    pieces = make_pieces()
    order = make_order(pieces, ny, nz)

    def per_device(x_in, grad_out, vectors, w_qkv, w_proj, w_fc1, b_fc1, w_fc2):
        n_micro, _, seq, width = x_in.shape
        mlp = w_fc1.shape[2]
        heads = w_proj.shape[1]
        pad = ((0, 0), (0, TOK - seq), (0, 0))
        x_p = jnp.pad(x_in.reshape(n_micro, seq, width), pad)
        go_p = jnp.pad(grad_out.reshape(n_micro, seq, width), pad)
        hbm, vmem = pl.BlockSpec(memory_space=pl.ANY), pl.BlockSpec(memory_space=pltpu.VMEM)
        n_img = 2 * n_micro
        act = lambda n, w: jax.ShapeDtypeStruct((n, TOK, w), BF16)
        flat = lambda f: jax.ShapeDtypeStruct((n_img, f, KEYS), BF16)
        dma, vm = pltpu.SemaphoreType.DMA, pltpu.VMEM
        outs = pl.pallas_call(
            functools.partial(pipeline_kernel, (seq, stages, n_micro)),
            name='pipeline',
            out_shape=[act(n_micro, width), act(n_micro, width), flat(width), flat(width), flat(width), flat(mlp // 2),
                       act(n_img, 3 * width // 2), act(n_img, mlp // 2), act(n_img, width // 2),
                       act(n_img, width), jax.ShapeDtypeStruct((2, 256, LANES), F32)],
            in_specs=[hbm, hbm, vmem, vmem, hbm, hbm, hbm, hbm],
            out_specs=[hbm] * 11,
            scratch_shapes=[
                vm((width, 3 * width), BF16), vm((width, width), BF16), vm((width, mlp), BF16), vm((mlp, width), BF16),
                vm((3 * width, width), BF16), vm((width, width), BF16), vm((mlp, width), BF16), vm((width, mlp), BF16),
                vm((n_micro, 3 * width + mlp, KEYS), BF16),
                vm((n_micro, TOK, width), BF16), vm((n_micro, TOK, width), BF16), vm((n_micro, TOK, width), BF16),
                vm((n_micro, TOK, width), BF16), vm((n_micro, TOK, width), BF16), vm((n_micro, KEYS, 3 * width), BF16),
                vm((n_micro, TOK, width), BF16), vm((n_micro, TOK, width), BF16), vm((n_micro, TOK, width), BF16),
                vm((n_micro, TOK, mlp), BF16), vm((n_micro, TOK, mlp), BF16), vm((n_micro, heads, TOK, KEYS), F32),
                vm((n_micro, 4, TOK, 1), F32), vm((n_micro, TOK, mlp), BF16), vm((n_micro, TOK, width), BF16),
                vm((TOK, width), BF16), vm((n_micro, TOK, 3 * width), BF16), vm((256, LANES), F32),
                dma((4,)), dma((2 * n_micro,)), dma((2 * n_micro,)), dma((2 * n_micro,)), dma((n_micro, 10)),
                dma((n_micro, 8)), dma((n_micro, 8)), dma((3,)),
            ],
            compiler_params=pltpu.CompilerParams(collective_id=0, has_side_effects=True, vmem_limit_bytes=67043328),
        )(x_p, go_p, vectors[0], b_fc1, w_qkv[0], w_proj[0].reshape(width, width), w_fc1[0], w_fc2[0])
        so, sg, xa1, xa2, xo, xf, dqkv, dz, dr, gy, vec = outs

        half = {'fc1': mlp // 2, 'fc2': width, 'qkv': 3 * width // 2, 'proj': width // 2}
        feats = {'fc1': width, 'fc2': mlp // 2, 'qkv': width, 'proj': width}
        names = ('fc1', 'fc2', 'qkv', 'proj')
        f32 = lambda *s: jax.ShapeDtypeStruct(s, F32)
        slots = [[], []]
        for name, _, _, cols in pieces:
            n1, n2 = (ny, nz) if FIRST_Y[name] else (nz, ny)
            slots[0].append(vm((n1, ROWS[name] // n1, cols), F32))
            slots[1].append(vm((n2, ROWS[name] // (n1 * n2), cols), F32))
        grads = pl.pallas_call(
            functools.partial(grad_kernel, (ny, nz, n_img, pieces, order)),
            name='gradients',
            out_shape=[f32(width, mlp), f32(mlp, width), f32(width, 3 * width), f32(width, width), f32(256, LANES)],
            in_specs=[hbm] * 9,
            out_specs=[hbm] * 5,
            scratch_shapes=(
                [vm((n_img, feats[n], KEYS), BF16) for n in names] + [vm((n_img, KEYS, half[n]), BF16) for n in names] + [vm((2, 256, LANES), F32)]
                + [vm((feats[n], half[n]), F32) for n in names] + [vm((256, LANES), F32)] + slots[0] + slots[1]
                + [dma((5, 2, n_img)), dma((4 * len(pieces),)), dma((len([o for o in order if o[0] == 'send']),)),
                   dma((len(pieces),)), dma((len(pieces),)), dma((len(pieces),))]),
            compiler_params=pltpu.CompilerParams(collective_id=1, has_side_effects=True, vmem_limit_bytes=63 * 1024 * 1024),
        )(xa2, xf, xa1, xo, dz, gy, dqkv, dr, vec)
        g_fc1, g_fc2, g_qkv, g_proj, g_vec = grads
        n_vec = vectors.shape[1] * width // LANES
        g_vectors = g_vec[:n_vec].reshape(1, vectors.shape[1], width)
        g_bfc1 = g_vec[n_vec:n_vec + mlp // LANES].reshape(1, mlp)
        return (so[:, :seq].reshape(1, n_micro, 1, seq, width), sg[:, :seq].reshape(1, n_micro, 1, seq, width), g_vectors,
                g_qkv[None], g_proj.reshape(1, heads, width // heads, width), g_fc1[None], g_bfc1, g_fc2[None])

    return jax.shard_map(per_device, mesh=mesh, in_specs=(act_spec, act_spec) + (stage_spec,) * 6,
                         out_specs=(out_act_spec, out_act_spec) + (stage_spec,) * 6, check_vma=False)
```

```python
import functools
import heapq
import math
import jax
import jax.numpy as jnp
from jax import lax
from jax.experimental import pallas as pl
from jax.experimental.pallas import tpu as pltpu
from jax.sharding import PartitionSpec as P

MESH = pl.DeviceIdType.MESH
F32 = jnp.float32
BF16 = jnp.bfloat16
TOK = 208
KEYS = 256
SENT = 200
LANES = 128
HEAD = 64
WIDE = 512
SPLIT = 112
SHIFT = 6200


def dot_nn(a, b):
    return jnp.dot(a, b, preferred_element_type=F32)


def dot_nt(a, b):
    return lax.dot_general(a, b, (((1,), (1,)), ((), ())), preferred_element_type=F32)


def rounded(x):
    return x.astype(BF16).astype(F32)


def aligned(start, size):
    return pl.ds(pl.multiple_of(start, LANES), size)


def row_sum(x):
    return jnp.sum(x, axis=-1, keepdims=True)


def col_sum(x):
    return jnp.sum(x.astype(F32), axis=0, keepdims=True)


def loop(n, body):
    def step(i, c):
        body(i)
        return c
    lax.fori_loop(0, n, step, 0)


def tiles(total):
    wide = total - total % WIDE
    out = [(slice(0, TOK), slice(c, c + WIDE)) for c in range(0, wide, WIDE)]
    if wide < total:
        out += [(rows, slice(wide, total)) for rows in (slice(0, SPLIT), slice(SPLIT, TOK))]
    return out


def pipeline_kernel(cfg, x_in, go_in, vec_ref, bf1_ref, wqkv_in, wproj_in, w1_in, w2_in,
                    so_out, sg_out, xa1, xa2, xo, xf, dqkv_out, dz_out, dr_out, gy_out, vec_out,
                    wqkv, wproj, w1, w2, wqkv_t, wproj_t, w1_t, w2_t, xt, x_raw, g_raw,
                    hbuf, gbuf, obuf, gibuf, a1, qkv, att, res, a2, zact, fact, prob, prob16, stats,
                    dz, dres, datt, gtmp, dqkv, raw16, ds16, vsum,
                    w_sem, in_sem, send_sem, recv_sem, loc_sem, psend_sem, precv_sem, vec_sem):
    seq, stages, n_micro = cfg
    width = wproj.shape[0]
    mlp = w1.shape[1]
    pairs = width // LANES
    half_qkv, half_mlp, half_w = 3 * width // 2, mlp // 2, width // 2
    dp = lax.axis_index('dp')
    stage = lax.axis_index('pp')
    core = lax.rem(dp, 2)
    mate = dp + 1 - 2 * core
    cores = (core, 1 - core)
    last = stages - 1
    nxt = lax.rem(stage + 1, stages)
    prv = lax.rem(stage + last, stages)
    at_first, at_last = pl.when(stage == 0), pl.when(stage == last)
    past_first, before_last = pl.when(stage > 0), pl.when(stage < last)
    remote = functools.partial(pltpu.make_async_remote_copy, device_id_type=MESH)

    loads = [pltpu.make_async_copy(src, dst, w_sem.at[i])
             for i, (src, dst) in enumerate(((wqkv_in, wqkv), (wproj_in, wproj), (w1_in, w1), (w2_in, w2)))]
    x_load = pltpu.make_async_copy(x_in, x_raw, in_sem.at[0])
    g_load = pltpu.make_async_copy(go_in, g_raw, in_sem.at[1])

    def split(raw, dst):
        for m in range(n_micro):
            dst[m, :seq] = raw[:, m, :]
            dst[m, seq:] = jnp.zeros((TOK - seq, width), BF16)

    at_first(x_load.start)
    for ld in loads:
        ld.start()
    at_last(g_load.start)

    barrier = pltpu.get_barrier_semaphore()
    for dev in ({'pp': nxt}, {'pp': prv}, {'dp': mate}):
        pl.semaphore_signal(barrier, device_id=dev, device_id_type=MESH)
    qkv[:, TOK:, :] = jnp.zeros((n_micro, KEYS - TOK, 3 * width), BF16)
    datt[TOK:, :] = jnp.zeros((KEYS - TOK, width), BF16)
    for buf in (hbuf, gbuf):
        buf[:, SENT:, :] = jnp.zeros((n_micro, TOK - SENT, width), BF16)
    vsum[...] = jnp.zeros(vsum.shape, F32)
    pl.semaphore_wait(barrier, 3)

    @pl.when((stage == 0) & (core == 1))
    def _():
        pl.delay(SHIFT)

    def fwd_copy(m):
        return remote(obuf.at[m, :SENT], hbuf.at[m, :SENT], send_sem.at[m], recv_sem.at[m], device_id={'pp': nxt})

    def bwd_copy(m):
        return remote(gibuf.at[m, :SENT], gbuf.at[m, :SENT], send_sem.at[n_micro + m], recv_sem.at[n_micro + m], device_id={'pp': prv})

    def local(src, dst, m, i):
        return pltpu.make_async_copy(src, dst, loc_sem.at[m, i])

    def exports(m, first, whole, halved):
        loc, far = [], []
        for i, (src, dst) in enumerate(whole + halved, first):
            for c, out in zip(cores, (loc, far)):
                part = src(m, c) if callable(src) else src.at[m]
                out.append(local(part, dst.at[m], m, i) if out is loc else
                           remote(part, dst.at[n_micro + m], psend_sem.at[m, i], precv_sem.at[m, i], device_id={'dp': mate}))
        return loc, far

    def xt_rows(i):
        return lambda m, c: xt.at[m, i * width:(i + 1) * width]

    def fwd_exports(m):
        return exports(m, 0, [(xt_rows(i), dst) for i, dst in enumerate((xa1, xa2, xo))],
                       [(lambda m, c: xt.at[m, pl.ds(pl.multiple_of(3 * width + c * half_mlp, LANES), half_mlp)], xf)])

    def half_of(ref, size):
        return lambda m, c: ref.at[m, :, aligned(c * size, size)]

    def bwd_exports(m):
        return exports(m, 4, [(gbuf, gy_out)], [(half_of(dz, half_mlp), dz_out), (half_of(dres, half_w), dr_out),
                                                (half_of(dqkv, half_qkv), dqkv_out)])

    def out_copies(m):
        return local(obuf.at[m], so_out.at[m], m, 8), local(gibuf.at[m], sg_out.at[m], m, 9)

    def row(i):
        return vec_ref[i:i + 1, :].astype(F32)

    bias_qkv = jnp.concatenate([row(i) for i in (2, 3, 4)], axis=1)

    def norm(m, src, idx):
        mean = row_sum(src) * (1.0 / width)
        cen = src - mean
        rs = lax.rsqrt(row_sum(cen * cen) * (1.0 / width) + 1e-5)
        stats[m, 2 * idx] = mean
        stats[m, 2 * idx + 1] = rs
        return cen * rs

    def add_vec(i, val):
        for t in range(val.shape[1] // LANES):
            at = slice(i * pairs + t, i * pairs + t + 1)
            vsum[at, :] = vsum[at, :] + val[:, LANES * t:LANES * (t + 1)]

    lane = lax.broadcasted_iota(jnp.int32, (1, LANES), 1)
    head_mask = [ok.astype(F32).astype(BF16) for ok in (lane < HEAD, lane >= HEAD)]
    key_ok = lax.broadcasted_iota(jnp.int32, (TOK, KEYS), 1) < seq
    scale = 1.0 / math.sqrt(HEAD)
    n_tile = mlp // width

    def flip_weights():
        for src, dst in ((w2, w2_t), (w1, w1_t), (wproj, wproj_t), (wqkv, wqkv_t)):
            by_row = src.shape[0] > src.shape[1]

            def body(i, src=src, dst=dst, by_row=by_row):
                at = aligned(i * KEYS, KEYS)
                if by_row:
                    dst[:, at] = src[at, :].T
                else:
                    dst[at, :] = src[:, at].T
            loop(max(src.shape) // KEYS, body)

    def flip_acts(m):
        fill = jnp.zeros((KEYS - TOK, width), BF16)
        for i, src in enumerate((a1, a2, att)):
            xt[m, i * width:(i + 1) * width, :] = jnp.concatenate([src[m], fill], axis=0).T

        def body(j):
            rows = pl.ds(pl.multiple_of((3 + j) * width, LANES), width)
            xt[m, rows, :] = jnp.concatenate([fact[m, :, aligned(j * width, width)], fill], axis=0).T
        loop(n_tile, body)
        for c in sum(fwd_exports(m), []):
            c.start()

    def forward(m):
        @past_first
        def _():
            fwd_copy(m).wait_recv()

        def need(i):
            pl.when((m == 0) & (stage == 0))(loads[i].wait)

        a1[m] = (norm(m, hbuf[m].astype(F32), 0) * row(0) + row(1)).astype(BF16)
        need(0)
        for rows, cols in tiles(3 * width):
            qkv[m, rows, cols] = (dot_nn(a1[m, rows], wqkv[:, cols]) + bias_qkv[:, cols]).astype(BF16)

        def scores(p):
            q2 = qkv[m, :TOK, p * LANES:(p + 1) * LANES]
            k2 = qkv[m, :, width + p * LANES:width + (p + 1) * LANES]
            for e, mask in enumerate(head_mask):
                raw16[p % 2, e] = (dot_nt(q2 * mask, k2) * scale).astype(BF16)

        def soft(p):
            for e in range(2):
                s = jnp.where(key_ok, raw16[p % 2, e].astype(F32), -1e30)
                ex = jnp.exp(s - jnp.max(s, axis=-1, keepdims=True))
                pr = ex * (1.0 / row_sum(ex))
                prob[m, 2 * p + e] = pr
                prob16[m, 2 * p + e] = pr.astype(BF16)

        def values(p):
            v2 = qkv[m, :, 2 * width + p * LANES:2 * width + (p + 1) * LANES]
            o = [dot_nn(prob16[m, 2 * p + e], v2 * mask) for e, mask in enumerate(head_mask)]
            att[m, :, p * LANES:(p + 1) * LANES] = sum(o).astype(BF16)

        staggered(pairs, (scores, soft, values))
        need(1)
        for rows, cols in tiles(width):
            res[m, rows, cols] = (hbuf[m, rows, cols].astype(F32) + dot_nn(att[m, rows], wproj[:, cols])
                                  + row(5)[:, cols]).astype(BF16)
        a2[m] = (norm(m, res[m].astype(F32), 1) * row(6) + row(7)).astype(BF16)
        need(2)
        for rows, cols in tiles(mlp):
            z = (dot_nn(a2[m, rows], w1[:, cols]) + bf1_ref[:, cols].astype(F32)).astype(BF16)
            zact[m, rows, cols] = z
            z = z.astype(F32)
            fact[m, rows, cols] = (z * (0.5 + 0.5 * lax.erf(z * math.sqrt(0.5)))).astype(BF16)
        need(3)
        for rows, cols in tiles(width):
            obuf[m, rows, cols] = (res[m, rows, cols].astype(F32) + dot_nn(fact[m, rows], w2[:, cols])
                                   + row(8)[:, cols]).astype(BF16)

        @before_last
        def _():
            fwd_copy(m).start()
        out_copies(m)[0].start()

    def norm_back(m, src, idx, gain, vec_row, skip):
        rs = stats[m, 2 * idx + 1]
        xhat = (src - stats[m, 2 * idx]) * rs
        g = gtmp[...].astype(F32)
        gx = g * xhat
        add_vec(vec_row, col_sum(gx))
        add_vec(vec_row + 1, col_sum(g))
        m1 = row_sum(g * gain) * (1.0 / width)
        m2 = row_sum(gx * gain) * (1.0 / width)
        return (skip + rs * (g * gain - m1 - xhat * m2)).astype(BF16)

    def backward(m):
        @before_last
        def _():
            bwd_copy(m).wait_recv()

        for rows, cols in tiles(mlp):
            ga = rounded(dot_nn(gbuf[m, rows], w2_t[:, cols]))
            z = zact[m, rows, cols].astype(F32)
            cdf = 0.5 + 0.5 * lax.erf(z * math.sqrt(0.5))
            pdf_z = jnp.exp2(z * z * (-0.5 * math.log2(math.e))) * (z * (1.0 / math.sqrt(2.0 * math.pi)))
            dz[m, rows, cols] = (ga * (cdf + pdf_z)).astype(BF16)
        for rows, cols in tiles(width):
            gtmp[rows, cols] = dot_nn(dz[m, rows], w1_t[:, cols]).astype(BF16)
        dres[m] = norm_back(m, res[m].astype(F32), 1, row(6), 6, gbuf[m].astype(F32))
        for rows, cols in tiles(width):
            datt[rows, cols] = dot_nn(dres[m, rows], wproj_t[:, cols]).astype(BF16)

        def dprobs(p):
            do2 = datt[:TOK, p * LANES:(p + 1) * LANES]
            v2 = qkv[m, :, 2 * width + p * LANES:2 * width + (p + 1) * LANES]
            for e, mask in enumerate(head_mask):
                raw16[p % 2, e] = dot_nt(do2 * mask, v2).astype(BF16)

        def dscores(p):
            for e in range(2):
                pr, d = prob[m, 2 * p + e], raw16[p % 2, e].astype(F32)
                ds16[p % 2, e] = (pr * (d - row_sum(pr * d))).astype(BF16)

        def dheads(p):
            q_t = qkv[m, :, p * LANES:(p + 1) * LANES].T
            k2 = qkv[m, :, width + p * LANES:width + (p + 1) * LANES]
            do_t = datt[:, p * LANES:(p + 1) * LANES].T
            dq = sum(dot_nn(ds16[p % 2, e], k2 * mask) for e, mask in enumerate(head_mask)) * scale
            dk, dv = [jnp.concatenate([dot_nn(lhs[HEAD * e:HEAD * (e + 1), :TOK], rhs(e)) for e in range(2)], axis=0)
                      for lhs, rhs in ((q_t, lambda e: ds16[p % 2, e]), (do_t, lambda e: prob16[m, 2 * p + e]))]
            for i, val in enumerate((dq.astype(BF16), (dk * scale).astype(BF16).T[:TOK], dv.astype(BF16).T[:TOK])):
                dqkv[m, :, i * width + p * LANES:i * width + (p + 1) * LANES] = val

        staggered(pairs, (dprobs, dscores, dheads))
        for rows, cols in tiles(width):
            gtmp[rows, cols] = dot_nn(dqkv[m, rows], wqkv_t[:, cols]).astype(BF16)
        gibuf[m] = norm_back(m, hbuf[m].astype(F32), 0, row(0), 0, dres[m].astype(F32))

        @past_first
        def _():
            bwd_copy(m).start()
        for c in sum(bwd_exports(m), [out_copies(m)[1]]):
            c.start()

    @at_first
    def _():
        x_load.wait()
        split(x_raw, hbuf)

    @at_last
    def _():
        g_load.wait()
        split(g_raw, gbuf)

    @past_first
    def _():
        for ld in loads:
            ld.wait()
        flip_weights()
    loop(n_micro, forward)
    at_first(flip_weights)

    @before_last
    def _():
        loop(n_micro, flip_acts)
    loop(n_micro, backward)

    @at_last
    def _():
        loop(n_micro, flip_acts)

    def sums(m):
        for j in range(3):
            add_vec(2 + j, col_sum(dqkv[m, :, j * width:(j + 1) * width]))
        add_vec(5, col_sum(dres[m]))
        add_vec(8, col_sum(gbuf[m]))
        for j in range(n_tile):
            add_vec(9 + j, col_sum(dz[m, :, j * width:(j + 1) * width]))
    loop(n_micro, sums)

    vec_loc = pltpu.make_async_copy(vsum, vec_out.at[0], vec_sem.at[0])
    vec_far = remote(vsum, vec_out.at[1], vec_sem.at[1], vec_sem.at[2], device_id={'dp': mate})
    vec_loc.start()
    vec_far.start()
    for m in range(n_micro):
        before_last(fwd_copy(m).wait_send)
        past_first(bwd_copy(m).wait_send)
        for c in out_copies(m):
            c.wait()
        for loc, far in (fwd_exports(m), bwd_exports(m)):
            for c in loc + far:
                c.wait()
    vec_loc.wait()
    vec_far.wait()


def staggered(n, phases):
    for i in range(n + len(phases) - 1):
        for d, phase in reversed(list(enumerate(phases))):
            if 0 <= i - d < n:
                phase(i - d)


WEIGHTS = ('fc1', 'fc2', 'qkv', 'proj')
PIECE_ORDER = ('fc1', 'qkv', 'fc2', 'proj')
FIRST_Y = {'fc1': True, 'qkv': True, 'fc2': False, 'proj': False, 'vec': True}
ROWS = {'fc1': 768, 'qkv': 768, 'fc2': 1536, 'proj': 768, 'vec': 256}
PLUS = {'fc1': 6, 'qkv': 5, 'fc2': 3, 'proj': 2}
MINUS = {'fc1': 6, 'qkv': 4, 'fc2': 3, 'proj': 1}
WIDEST = {'fc1': 2, 'qkv': 2, 'fc2': 1, 'proj': 1}


def make_pieces():
    pieces = []
    for name in PIECE_ORDER:
        col = 0
        for way, tiles in ((1, PLUS[name]), (-1, MINUS[name])):
            k = -(-tiles // WIDEST[name])
            for i in range(k):
                t = tiles // k + (1 if i < tiles % k else 0)
                pieces.append((name, way, col * LANES, t * LANES))
                col += t
    return pieces + [('vec', 1, 0, LANES)]


def make_order(pieces, ny, nz, rate=51.3e3, lat=2.79, lat_y=0.3, first=5.0, ready=15.0, step=0.0736):
    heap, order, waiting, free, count = [], [], {}, {}, [0]

    def on_y(i, ph):
        return FIRST_Y[pieces[i][0]] == (ph == 1)

    def ring(i, ph):
        return ny if on_y(i, ph) else nz

    def nbytes(i, ph):
        rows = ROWS[pieces[i][0]] // ring(i, 1)
        return (rows if ph == 1 else rows // ring(i, 2)) * pieces[i][3] * 4

    def push(t, item):
        count[0] += 1
        heapq.heappush(heap, (t, count[0], item))

    def dispatch(t, key):
        queue = waiting.get(key)
        if queue and free.get(key, 0.0) <= t + 1e-9:
            typ, i, ph, k = heapq.heappop(queue)[-1]
            w = nbytes(i, ph) / rate
            free[key] = t + w
            order.append(('send', typ, i, ph, k))
            push(t + w, ('free', key))
            push(t + w + lat + (lat_y if key[0] else 0.0), ('land', (typ, i, ph, k)))

    def enqueue(t, typ, i, ph, k):
        way = pieces[i][1] * (1 if typ == 'rs' else -1)
        key = (on_y(i, ph), way)
        count[0] += 1
        heapq.heappush(waiting.setdefault(key, []), ((ph == 1 and typ == 'ag', ph == 1, -k if typ == 'rs' else 0, i), count[0], (typ, i, ph, k)))
        dispatch(t, key)

    for i in range(len(pieces)):
        push(first, ('start', i))
    seq = ready
    while heap:
        t, _, item = heapq.heappop(heap)
        if item[0] == 'free':
            dispatch(t, item[1])
        elif item[0] == 'start':
            enqueue(t, 'rs', item[1], 1, 0)
        elif item[0] == 'land':
            seq = max(seq, t) + step
            push(seq, ('done', item[1]))
        else:
            typ, i, ph, k = item[1]
            order.append(('recv', typ, i, ph, k))
            if k < ring(i, ph) - 2:
                enqueue(t, typ, i, ph, k + 1)
            elif typ == 'rs':
                enqueue(t, 'rs' if ph == 1 else 'ag', i, 2, 0)
            elif ph == 2:
                enqueue(t, 'ag', i, 1, 0)
    return order


def grad_kernel(cfg, *refs):
    ny, nz, n_img, pieces, order = cfg
    n_p = len(pieces)
    it = iter(refs)
    take = lambda n: [next(it) for _ in range(n)]
    names = WEIGHTS
    each = lambda: dict(zip(names, take(len(names))))
    x_in, y_in = each(), each()
    vec_in = next(it)
    acc = each()
    acc['vec'] = next(it)
    mated = each()
    x_t, y_v = each(), each()
    vec_v = next(it)
    slot1, slot2 = take(n_p), take(n_p)
    ld_sem, send_sem, recv_sem, mate_send, mate_recv = take(5)

    dp = lax.axis_index('dp')
    core = lax.rem(dp, 2)
    mate = dp + 1 - 2 * core
    py = lax.rem(lax.div(dp, 2), ny)
    pz = lax.div(dp, 2 * ny)

    def at(y, z):
        return (z * ny + y) * 2 + core

    def turn(pos, by, n):
        return lax.rem(pos + by % n, n)

    nbr = {(True, 1): at(turn(py, 1, ny), pz), (True, -1): at(turn(py, -1, ny), pz),
           (False, 1): at(py, turn(pz, 1, nz)), (False, -1): at(py, turn(pz, -1, nz))}

    loads = []
    for j, name in enumerate(names):
        for s in range(n_img):
            loads.append((name, pltpu.make_async_copy(x_in[name].at[s], x_t[name].at[s], ld_sem.at[j, 0, s])))
            loads.append((name, pltpu.make_async_copy(y_in[name].at[s], y_v[name].at[s, 0:TOK, :], ld_sem.at[j, 1, s])))
    vec_load = pltpu.make_async_copy(vec_in, vec_v, ld_sem.at[4, 0, 0])
    for _, ld in loads:
        ld.start()
    vec_load.start()

    barrier = pltpu.get_barrier_semaphore()
    for dev in list(nbr.values()) + [mate]:
        pl.semaphore_signal(barrier, device_id={'dp': dev}, device_id_type=MESH)

    for name in names:
        y_v[name][:, TOK:, :] = jnp.zeros((n_img, KEYS - TOK, y_v[name].shape[2]), BF16)
    pl.semaphore_wait(barrier, 5)

    def ring(i, ph):
        return ny if FIRST_Y[pieces[i][0]] == (ph == 1) else nz

    def place(i, ph):
        return py if FIRST_Y[pieces[i][0]] == (ph == 1) else pz

    def rows1(i, by):
        size = ROWS[pieces[i][0]] // ring(i, 1)
        return pl.ds(pl.multiple_of(turn(place(i, 1), by, ring(i, 1)) * size, 8), size)

    def rows2(i, by):
        big = ROWS[pieces[i][0]] // ring(i, 1)
        size = big // ring(i, 2)
        return pl.ds(pl.multiple_of(place(i, 1) * big + turn(place(i, 2), by, ring(i, 2)) * size, 8), size)

    def view(i, ph, by):
        name, _, col, cols = pieces[i]
        rows = rows1(i, by) if ph == 1 else rows2(i, by)
        return acc[name].at[rows, col:col + cols]

    steps = {}
    for _, typ, i, ph, k in order:
        steps.setdefault((typ, i, ph, k), len(steps))

    def landing(i, ph, k):
        n = ring(i, ph)
        return n - 3 - k if k <= n - 3 else n - 1

    def sent(group, i):
        slots = ((slot1, slot2)[group % 2])[i]
        part = slots.at[0:slots.shape[0] - 1]
        pltpu.make_async_copy(part, part, send_sem.at[group * n_p + i]).wait()

    def copy(typ, i, ph, k):
        way = pieces[i][1] * (1 if typ == 'rs' else -1)
        group = ((0 if typ == 'rs' else 2) + ph - 1) * n_p + i
        slots = (slot1 if ph == 1 else slot2)[i]
        if typ == 'rs':
            src, dst = view(i, ph, -way * (1 + k)), slots.at[k]
        else:
            src = slots.at[landing(i, ph, k - 1)] if k else view(i, ph, 0)
            dst = slots.at[landing(i, ph, k)]
        return pltpu.make_async_remote_copy(src, dst, send_sem.at[group], recv_sem.at[steps[typ, i, ph, k]],
                                            device_id={'dp': nbr[FIRST_Y[pieces[i][0]] == (ph == 1), way]}, device_id_type=MESH)

    def deliver(i, src, by):
        name, _, col, cols = pieces[i]
        if name != 'vec':
            pltpu.make_async_remote_copy(src, mated[name].at[rows1(i, by), col:col + cols], mate_send.at[i], mate_recv.at[i],
                                         device_id={'dp': mate}, device_id_type=MESH).start()

    def multiply(k, name):
        i = next(j for j in range(n_p) if pieces[j][0] == name)
        size = ROWS[name] // ring(i, 1)
        split = PLUS[name] * LANES
        for way, cols in ((1, slice(0, split)), (-1, slice(split, split + MINUS[name] * LANES))):
            idx = lax.rem(place(i, 1) + (2 * ring(i, 1) - way) - way * k, ring(i, 1))
            rows = pl.ds(pl.multiple_of(idx * size, 8), size)
            acc[name][rows, cols] = sum(dot_nn(x_t[name][s, rows, :], y_v[name][s, :, cols]) for s in range(n_img))

    n_first = next(j for j, o in enumerate(order) if o[0] == 'recv')
    begin, todo = order[:n_first], order[n_first:]
    for name in ('vec',) + names:
        if name == 'vec':
            vec_load.wait()
            acc['vec'][...] = vec_v[0] + vec_v[1]
        else:
            for nm, ld in loads:
                if nm == name:
                    ld.wait()
            multiply(0, name)
        for o in begin:
            if pieces[o[2]][0] == name:
                copy(*o[1:]).start()
    for name in names:
        i = next(j for j in range(n_p) if pieces[j][0] == name)
        loop(ring(i, 1) - 1, lambda k, name=name: multiply(k + 1, name))

    for what, typ, i, ph, k in todo:
        if what == 'send':
            copy(typ, i, ph, k).start()
            continue
        copy(typ, i, ph, k).wait_recv()
        way = pieces[i][1] * (1 if typ == 'rs' else -1)
        if typ == 'rs':
            dst = view(i, ph, -way * (2 + k))
            dst[...] = dst[...] + (slot1 if ph == 1 else slot2)[i][k]
        elif ph == 1:
            slot = landing(i, 1, k)
            deliver(i, slot1[i].at[slot], -way * (1 + k))
            if k == 0:
                sent(0, i)
            dst = view(i, 1, -way * (1 + k))
            dst[...] = slot1[i][slot]
        elif k == ring(i, 2) - 2:
            sent(1, i)
            for j in range(ring(i, 2) - 1):
                dst = view(i, 2, -way * (1 + j))
                dst[...] = slot2[i][landing(i, 2, j)]
            deliver(i, view(i, 1, 0), 0)

    for i in range(n_p):
        name, _, col, cols = pieces[i]
        for group in (2, 3):
            sent(group, i)
        whole = acc[name].at[:, col:col + cols]
        if name != 'vec':
            pltpu.make_async_copy(whole, whole, mate_send.at[i]).wait()
            pltpu.make_async_copy(whole, whole, mate_recv.at[i]).wait()


def output_kernel(parts, *refs):
    it = iter(refs)
    take = lambda n: [next(it) for _ in range(n)]
    names = WEIGHTS
    n = len(names)
    own, vec, mated, acts = take(n), next(it), take(n), take(2)
    out, g_vec, g_b, joined = take(n), next(it), next(it), take(2)
    act_v, join_v, sem, act_sem = take(2), take(2), *take(2)
    core = lax.rem(lax.axis_index('dp'), 2)
    copies = []
    for j, name in enumerate(names):
        for c, src in ((core, own[j]), (1 - core, mated[j])):
            rows, cols = src.shape
            step = rows // parts[name]
            for r in range(0, rows, step):
                if name == 'fc2':
                    dst = out[j].at[pl.ds(pl.multiple_of(c * rows + r, 8), step), :]
                else:
                    dst = out[j].at[r:r + step, aligned(c * cols, cols)]
                copies.append(pltpu.make_async_copy(src.at[r:r + step], dst, sem.at[len(copies)]))
    reads = [pltpu.make_async_copy(acts[k], act_v[k], act_sem.at[k]) for k in range(2)]
    writes = [pltpu.make_async_copy(join_v[k], joined[k], act_sem.at[2 + k]) for k in range(2)]
    for c in reads + copies:
        c.start()
    n_vec, width = g_vec.shape
    per = width // LANES
    for i in range(n_vec):
        for t in range(per):
            g_vec[i:i + 1, t * LANES:(t + 1) * LANES] = vec[i * per + t:i * per + t + 1, :]
    for t in range(g_b.shape[1] // LANES):
        g_b[:, t * LANES:(t + 1) * LANES] = vec[n_vec * per + t:n_vec * per + t + 1, :]
    for k in range(2):
        reads[k].wait()
        for m in range(join_v[k].shape[1]):
            join_v[k][:, m, :] = act_v[k][m, 0:join_v[k].shape[0]]
        writes[k].start()
    for c in copies + writes:
        c.wait()


def solution(mesh):
    stages = mesh.shape['pp']
    n_dp = mesh.shape['dp']
    ny = 4 if n_dp == 64 else 2
    nz = n_dp // (2 * ny)
    act_spec = P(None, 'dp')
    stage_spec = P('pp')
    out_act_spec = P('pp', None, 'dp')
    pieces = make_pieces()
    order = make_order(pieces, ny, nz)

    def per_device(x_in, grad_out, vectors, w_qkv, w_proj, w_fc1, b_fc1, w_fc2):
        n_micro, _, seq, width = x_in.shape
        mlp = w_fc1.shape[2]
        heads = w_proj.shape[1]
        x_p = x_in.reshape(n_micro, seq, width).transpose(1, 0, 2)
        go_p = grad_out.reshape(n_micro, seq, width).transpose(1, 0, 2)
        hbm, vmem = pl.BlockSpec(memory_space=pl.ANY), pl.BlockSpec(memory_space=pltpu.VMEM)
        n_img = 2 * n_micro
        act = lambda n, w: jax.ShapeDtypeStruct((n, TOK, w), BF16)
        flat = lambda f: jax.ShapeDtypeStruct((n_img, f, KEYS), BF16)
        dma, vm = pltpu.SemaphoreType.DMA, pltpu.VMEM
        outs = pl.pallas_call(
            functools.partial(pipeline_kernel, (seq, stages, n_micro)),
            name='pipeline',
            out_shape=[act(n_micro, width), act(n_micro, width), flat(width), flat(width), flat(width), flat(mlp // 2),
                       act(n_img, 3 * width // 2), act(n_img, mlp // 2), act(n_img, width // 2),
                       act(n_img, width), jax.ShapeDtypeStruct((2, 256, LANES), F32)],
            in_specs=[hbm, hbm, vmem, vmem, hbm, hbm, hbm, hbm],
            out_specs=[hbm] * 11,
            scratch_shapes=[
                vm((width, 3 * width), BF16), vm((width, width), BF16), vm((width, mlp), BF16), vm((mlp, width), BF16),
                vm((3 * width, width), BF16), vm((width, width), BF16), vm((mlp, width), BF16), vm((width, mlp), BF16),
                vm((n_micro, 3 * width + mlp, KEYS), BF16),
                vm((seq, n_micro, width), BF16), vm((seq, n_micro, width), BF16),
                vm((n_micro, TOK, width), BF16), vm((n_micro, TOK, width), BF16), vm((n_micro, TOK, width), BF16),
                vm((n_micro, TOK, width), BF16), vm((n_micro, TOK, width), BF16), vm((n_micro, KEYS, 3 * width), BF16),
                vm((n_micro, TOK, width), BF16), vm((n_micro, TOK, width), BF16), vm((n_micro, TOK, width), BF16),
                vm((n_micro, TOK, mlp), BF16), vm((n_micro, TOK, mlp), BF16), vm((n_micro, heads, TOK, KEYS), F32),
                vm((n_micro, heads, TOK, KEYS), BF16),
                vm((n_micro, 4, TOK, 1), F32), vm((n_micro, TOK, mlp), BF16), vm((n_micro, TOK, width), BF16),
                vm((KEYS, width), BF16), vm((TOK, width), BF16), vm((n_micro, TOK, 3 * width), BF16),
                vm((2, 2, TOK, KEYS), BF16), vm((2, 2, TOK, KEYS), BF16), vm((KEYS, LANES), F32),
                dma((4,)), dma((2,)), dma((2 * n_micro,)), dma((2 * n_micro,)), dma((n_micro, 10)),
                dma((n_micro, 8)), dma((n_micro, 8)), dma((3,)),
            ],
            compiler_params=pltpu.CompilerParams(collective_id=0, has_side_effects=True, vmem_limit_bytes=67043328),
        )(x_p, go_p, vectors[0], b_fc1, w_qkv[0], w_proj[0].reshape(width, width), w_fc1[0], w_fc2[0])
        so, sg, xa1, xa2, xo, xf, dqkv, dz, dr, gy, vec = outs

        half = {'fc1': mlp // 2, 'fc2': width, 'qkv': 3 * width // 2, 'proj': width // 2}
        feats = {'fc1': width, 'fc2': mlp // 2, 'qkv': width, 'proj': width}
        names = WEIGHTS
        f32 = lambda *s: jax.ShapeDtypeStruct(s, F32)
        slots = [[], []]
        for name, _, _, cols in pieces:
            n1, n2 = (ny, nz) if FIRST_Y[name] else (nz, ny)
            slots[0].append(vm((n1, ROWS[name] // n1, cols), F32))
            slots[1].append(vm((n2, ROWS[name] // (n1 * n2), cols), F32))
        grads = pl.pallas_call(
            functools.partial(grad_kernel, (ny, nz, n_img, pieces, order)),
            name='gradients',
            out_shape=[vm((feats[n], half[n]), F32) for n in names] + [vm((256, LANES), F32)]
            + [vm((feats[n], half[n]), F32) for n in names],
            in_specs=[hbm] * 9,
            out_specs=[vmem] * 9,
            scratch_shapes=(
                [vm((n_img, feats[n], KEYS), BF16) for n in names] + [vm((n_img, KEYS, half[n]), BF16) for n in names]
                + [vm((2, 256, LANES), F32)] + slots[0] + slots[1]
                + [dma((5, 2, n_img)), dma((4 * len(pieces),)), dma((len([o for o in order if o[0] == 'send']),)),
                   dma((len(pieces),)), dma((len(pieces),))]),
            compiler_params=pltpu.CompilerParams(collective_id=1, has_side_effects=True, vmem_limit_bytes=35 * 1024 * 1024),
        )(xa2, xf, xa1, xo, dz, gy, dqkv, dr, vec)
        parts = {'fc1': 3, 'fc2': 3, 'qkv': 3, 'proj': 1}
        raw = jax.ShapeDtypeStruct((seq, n_micro, width), BF16)
        g_fc1, g_fc2, g_qkv, g_proj, g_vectors, g_bfc1, so, sg = pl.pallas_call(
            functools.partial(output_kernel, parts),
            name='outputs',
            out_shape=[f32(width, mlp), f32(mlp, width), f32(width, 3 * width), f32(width, width), f32(vectors.shape[1], width),
                       f32(1, mlp), raw, raw],
            in_specs=[vmem] * 9 + [hbm] * 2,
            out_specs=[hbm] * 4 + [vmem] * 2 + [hbm] * 2,
            scratch_shapes=[vm((n_micro, TOK, width), BF16)] * 2 + [vm((seq, n_micro, width), BF16)] * 2
            + [dma((2 * sum(parts.values()),)), dma((4,))],
            compiler_params=pltpu.CompilerParams(vmem_limit_bytes=5 * 1024 * 1024),
        )(*grads, so, sg)
        so, sg = [t.transpose(1, 0, 2).reshape(1, n_micro, 1, seq, width) for t in (so, sg)]
        return (so, sg, g_vectors[None], g_qkv[None], g_proj.reshape(1, heads, width // heads, width), g_fc1[None], g_bfc1,
                g_fc2[None])

    return jax.shard_map(per_device, mesh=mesh, in_specs=(act_spec, act_spec) + (stage_spec,) * 6,
                         out_specs=(out_act_spec, out_act_spec) + (stage_spec,) * 6, check_vma=False)
```

```python
import functools
import heapq
import math
import jax
import jax.numpy as jnp
from jax import lax
from jax.experimental import pallas as pl
from jax.experimental.pallas import tpu as pltpu
from jax.sharding import PartitionSpec as P

MESH = pl.DeviceIdType.MESH
F32 = jnp.float32
BF16 = jnp.bfloat16
TOK = 208
KEYS = 256
SENT = 200
LANES = 128
HEAD = 64
WIDE = 512
SPLIT = 112
SHIFT = 6200


def dot_nn(a, b):
    return jnp.dot(a, b, preferred_element_type=F32)


def dot_nt(a, b):
    return lax.dot_general(a, b, (((1,), (1,)), ((), ())), preferred_element_type=F32)


def rounded(x):
    return x.astype(BF16).astype(F32)


def aligned(start, size):
    return pl.ds(pl.multiple_of(start, LANES), size)


def row_sum(x):
    return jnp.sum(x, axis=-1, keepdims=True)


def col_sum(x):
    return jnp.sum(x.astype(F32), axis=0, keepdims=True)


def loop(n, body):
    def step(i, c):
        body(i)
        return c
    lax.fori_loop(0, n, step, 0)


def tiles(total):
    wide = total - total % WIDE
    out = [(slice(0, TOK), slice(c, c + WIDE)) for c in range(0, wide, WIDE)]
    if wide < total:
        out += [(rows, slice(wide, total)) for rows in (slice(0, SPLIT), slice(SPLIT, TOK))]
    return out


def pipeline_kernel(cfg, x_in, go_in, vec_ref, bf1_ref, wqkv_in, wproj_in, w1_in, w2_in,
                    so_out, sg_out, xa1, xa2, xo, xf, dqkv_out, dz_out, dr_out, gy_out, vec_out,
                    wqkv, wproj, w1, w2, wqkv_t, wproj_t, w1_t, w2_t, xt, x_raw, g_raw,
                    hbuf, gbuf, obuf, gibuf, a1, qkv, att, res, a2, zact, fact, prob, prob16, stats,
                    dz, dres, datt, gtmp, dqkv, raw16, ds16, vsum,
                    w_sem, in_sem, send_sem, recv_sem, loc_sem, psend_sem, precv_sem, vec_sem):
    seq, stages, n_micro = cfg
    width = wproj.shape[0]
    mlp = w1.shape[1]
    pairs = width // LANES
    half_qkv, half_mlp, half_w = 3 * width // 2, mlp // 2, width // 2
    dp = lax.axis_index('dp')
    stage = lax.axis_index('pp')
    core = lax.rem(dp, 2)
    mate = dp + 1 - 2 * core
    cores = (core, 1 - core)
    last = stages - 1
    nxt = lax.rem(stage + 1, stages)
    prv = lax.rem(stage + last, stages)
    at_first, at_last = pl.when(stage == 0), pl.when(stage == last)
    past_first, before_last = pl.when(stage > 0), pl.when(stage < last)
    remote = functools.partial(pltpu.make_async_remote_copy, device_id_type=MESH)

    loads = [pltpu.make_async_copy(src, dst, w_sem.at[i])
             for i, (src, dst) in enumerate(((wqkv_in, wqkv), (wproj_in, wproj), (w1_in, w1), (w2_in, w2)))]
    x_load = pltpu.make_async_copy(x_in, x_raw, in_sem.at[0])
    g_load = pltpu.make_async_copy(go_in, g_raw, in_sem.at[1])

    def split(raw, dst):
        for m in range(n_micro):
            dst[m, :seq] = raw[:, m, :]
            dst[m, seq:] = jnp.zeros((TOK - seq, width), BF16)

    at_first(x_load.start)
    for ld in loads:
        ld.start()
    at_last(g_load.start)

    barrier = pltpu.get_barrier_semaphore()
    for dev in ({'pp': nxt}, {'pp': prv}, {'dp': mate}):
        pl.semaphore_signal(barrier, device_id=dev, device_id_type=MESH)
    qkv[:, TOK:, :] = jnp.zeros((n_micro, KEYS - TOK, 3 * width), BF16)
    datt[TOK:, :] = jnp.zeros((KEYS - TOK, width), BF16)
    for buf in (hbuf, gbuf):
        buf[:, SENT:, :] = jnp.zeros((n_micro, TOK - SENT, width), BF16)
    vsum[...] = jnp.zeros(vsum.shape, F32)
    pl.semaphore_wait(barrier, 3)

    @pl.when((stage == 0) & (core == 1))
    def _():
        pl.delay(SHIFT)

    def fwd_copy(m):
        return remote(obuf.at[m, :SENT], hbuf.at[m, :SENT], send_sem.at[m], recv_sem.at[m], device_id={'pp': nxt})

    def bwd_copy(m):
        return remote(gibuf.at[m, :SENT], gbuf.at[m, :SENT], send_sem.at[n_micro + m], recv_sem.at[n_micro + m], device_id={'pp': prv})

    def local(src, dst, m, i):
        return pltpu.make_async_copy(src, dst, loc_sem.at[m, i])

    def exports(m, first, whole, halved):
        loc, far = [], []
        for i, (src, dst) in enumerate(whole + halved, first):
            for c, out in zip(cores, (loc, far)):
                part = src(m, c) if callable(src) else src.at[m]
                out.append(local(part, dst.at[m], m, i) if out is loc else
                           remote(part, dst.at[n_micro + m], psend_sem.at[m, i], precv_sem.at[m, i], device_id={'dp': mate}))
        return loc, far

    def xt_rows(i):
        return lambda m, c: xt.at[m, i * width:(i + 1) * width]

    def fwd_exports(m):
        return exports(m, 0, [(xt_rows(i), dst) for i, dst in enumerate((xa1, xa2, xo))],
                       [(lambda m, c: xt.at[m, pl.ds(pl.multiple_of(3 * width + c * half_mlp, LANES), half_mlp)], xf)])

    def half_of(ref, size):
        return lambda m, c: ref.at[m, :, aligned(c * size, size)]

    def bwd_exports(m):
        return exports(m, 4, [(gbuf, gy_out)], [(half_of(dz, half_mlp), dz_out), (half_of(dres, half_w), dr_out),
                                                (half_of(dqkv, half_qkv), dqkv_out)])

    def out_copies(m):
        return local(obuf.at[m], so_out.at[m], m, 8), local(gibuf.at[m], sg_out.at[m], m, 9)

    def row(i):
        return vec_ref[i:i + 1, :].astype(F32)

    bias_qkv = jnp.concatenate([row(i) for i in (2, 3, 4)], axis=1)

    def norm(m, src, idx):
        mean = row_sum(src) * (1.0 / width)
        cen = src - mean
        rs = lax.rsqrt(row_sum(cen * cen) * (1.0 / width) + 1e-5)
        stats[m, 2 * idx] = mean
        stats[m, 2 * idx + 1] = rs
        return cen * rs

    def add_vec(i, val):
        for t in range(val.shape[1] // LANES):
            at = slice(i * pairs + t, i * pairs + t + 1)
            vsum[at, :] = vsum[at, :] + val[:, LANES * t:LANES * (t + 1)]

    lane = lax.broadcasted_iota(jnp.int32, (1, LANES), 1)
    head_mask = [ok.astype(F32).astype(BF16) for ok in (lane < HEAD, lane >= HEAD)]
    key_ok = lax.broadcasted_iota(jnp.int32, (TOK, KEYS), 1) < seq
    scale = 1.0 / math.sqrt(HEAD)
    n_tile = mlp // width

    def flip_weights():
        for src, dst in ((w2, w2_t), (w1, w1_t), (wproj, wproj_t), (wqkv, wqkv_t)):
            by_row = src.shape[0] > src.shape[1]

            def body(i, src=src, dst=dst, by_row=by_row):
                at = aligned(i * KEYS, KEYS)
                if by_row:
                    dst[:, at] = src[at, :].T
                else:
                    dst[at, :] = src[:, at].T
            loop(max(src.shape) // KEYS, body)

    def flip_acts(m):
        fill = jnp.zeros((KEYS - TOK, width), BF16)
        for i, src in enumerate((a1, a2, att)):
            xt[m, i * width:(i + 1) * width, :] = jnp.concatenate([src[m], fill], axis=0).T

        def body(j):
            rows = pl.ds(pl.multiple_of((3 + j) * width, LANES), width)
            xt[m, rows, :] = jnp.concatenate([fact[m, :, aligned(j * width, width)], fill], axis=0).T
        loop(n_tile, body)
        for c in sum(fwd_exports(m), []):
            c.start()

    def forward(m):
        @past_first
        def _():
            fwd_copy(m).wait_recv()

        def need(i):
            pl.when((m == 0) & (stage == 0))(loads[i].wait)

        a1[m] = (norm(m, hbuf[m].astype(F32), 0) * row(0) + row(1)).astype(BF16)
        need(0)
        for rows, cols in tiles(3 * width):
            qkv[m, rows, cols] = (dot_nn(a1[m, rows], wqkv[:, cols]) + bias_qkv[:, cols]).astype(BF16)

        def scores(p):
            q2 = qkv[m, :TOK, p * LANES:(p + 1) * LANES]
            k2 = qkv[m, :, width + p * LANES:width + (p + 1) * LANES]
            for e, mask in enumerate(head_mask):
                raw16[p % 2, e] = (dot_nt(q2 * mask, k2) * scale).astype(BF16)

        def soft(p):
            for e in range(2):
                s = jnp.where(key_ok, raw16[p % 2, e].astype(F32), -1e30)
                ex = jnp.exp(s - jnp.max(s, axis=-1, keepdims=True))
                pr = ex * (1.0 / row_sum(ex))
                prob[m, 2 * p + e] = pr
                prob16[m, 2 * p + e] = pr.astype(BF16)

        def values(p):
            v2 = qkv[m, :, 2 * width + p * LANES:2 * width + (p + 1) * LANES]
            o = [dot_nn(prob16[m, 2 * p + e], v2 * mask) for e, mask in enumerate(head_mask)]
            att[m, :, p * LANES:(p + 1) * LANES] = sum(o).astype(BF16)

        staggered(pairs, (scores, soft, values))
        need(1)
        for rows, cols in tiles(width):
            res[m, rows, cols] = (hbuf[m, rows, cols].astype(F32) + dot_nn(att[m, rows], wproj[:, cols])
                                  + row(5)[:, cols]).astype(BF16)
        a2[m] = (norm(m, res[m].astype(F32), 1) * row(6) + row(7)).astype(BF16)
        need(2)
        for rows, cols in tiles(mlp):
            z = (dot_nn(a2[m, rows], w1[:, cols]) + bf1_ref[:, cols].astype(F32)).astype(BF16)
            zact[m, rows, cols] = z
            z = z.astype(F32)
            fact[m, rows, cols] = (z * (0.5 + 0.5 * lax.erf(z * math.sqrt(0.5)))).astype(BF16)
        need(3)
        for rows, cols in tiles(width):
            obuf[m, rows, cols] = (res[m, rows, cols].astype(F32) + dot_nn(fact[m, rows], w2[:, cols])
                                   + row(8)[:, cols]).astype(BF16)

        @before_last
        def _():
            fwd_copy(m).start()
        out_copies(m)[0].start()

    def norm_back(m, src, idx, gain, vec_row, skip):
        rs = stats[m, 2 * idx + 1]
        xhat = (src - stats[m, 2 * idx]) * rs
        g = gtmp[...].astype(F32)
        gx = g * xhat
        add_vec(vec_row, col_sum(gx))
        add_vec(vec_row + 1, col_sum(g))
        m1 = row_sum(g * gain) * (1.0 / width)
        m2 = row_sum(gx * gain) * (1.0 / width)
        return (skip + rs * (g * gain - m1 - xhat * m2)).astype(BF16)

    def backward(m):
        @before_last
        def _():
            bwd_copy(m).wait_recv()

        for rows, cols in tiles(mlp):
            ga = rounded(dot_nn(gbuf[m, rows], w2_t[:, cols]))
            z = zact[m, rows, cols].astype(F32)
            cdf = 0.5 + 0.5 * lax.erf(z * math.sqrt(0.5))
            pdf_z = jnp.exp2(z * z * (-0.5 * math.log2(math.e))) * (z * (1.0 / math.sqrt(2.0 * math.pi)))
            dz[m, rows, cols] = (ga * (cdf + pdf_z)).astype(BF16)
        for rows, cols in tiles(width):
            gtmp[rows, cols] = dot_nn(dz[m, rows], w1_t[:, cols]).astype(BF16)
        dres[m] = norm_back(m, res[m].astype(F32), 1, row(6), 6, gbuf[m].astype(F32))
        for rows, cols in tiles(width):
            datt[rows, cols] = dot_nn(dres[m, rows], wproj_t[:, cols]).astype(BF16)

        def dprobs(p):
            do2 = datt[:TOK, p * LANES:(p + 1) * LANES]
            v2 = qkv[m, :, 2 * width + p * LANES:2 * width + (p + 1) * LANES]
            for e, mask in enumerate(head_mask):
                raw16[p % 2, e] = dot_nt(do2 * mask, v2).astype(BF16)

        def dscores(p):
            for e in range(2):
                pr, d = prob[m, 2 * p + e], raw16[p % 2, e].astype(F32)
                ds16[p % 2, e] = (pr * (d - row_sum(pr * d))).astype(BF16)

        def dheads(p):
            q_t = qkv[m, :, p * LANES:(p + 1) * LANES].T
            k2 = qkv[m, :, width + p * LANES:width + (p + 1) * LANES]
            do_t = datt[:, p * LANES:(p + 1) * LANES].T
            dq = sum(dot_nn(ds16[p % 2, e], k2 * mask) for e, mask in enumerate(head_mask)) * scale
            dk, dv = [jnp.concatenate([dot_nn(lhs[HEAD * e:HEAD * (e + 1), :TOK], rhs(e)) for e in range(2)], axis=0)
                      for lhs, rhs in ((q_t, lambda e: ds16[p % 2, e]), (do_t, lambda e: prob16[m, 2 * p + e]))]
            for i, val in enumerate((dq.astype(BF16), (dk * scale).astype(BF16).T[:TOK], dv.astype(BF16).T[:TOK])):
                dqkv[m, :, i * width + p * LANES:i * width + (p + 1) * LANES] = val

        staggered(pairs, (dprobs, dscores, dheads))
        for rows, cols in tiles(width):
            gtmp[rows, cols] = dot_nn(dqkv[m, rows], wqkv_t[:, cols]).astype(BF16)
        gibuf[m] = norm_back(m, hbuf[m].astype(F32), 0, row(0), 0, dres[m].astype(F32))

        @past_first
        def _():
            bwd_copy(m).start()
        for c in sum(bwd_exports(m), [out_copies(m)[1]]):
            c.start()

    @at_first
    def _():
        x_load.wait()
        split(x_raw, hbuf)

    @at_last
    def _():
        g_load.wait()
        split(g_raw, gbuf)

    @past_first
    def _():
        for ld in loads:
            ld.wait()
        flip_weights()
    loop(n_micro, forward)
    at_first(flip_weights)

    @before_last
    def _():
        loop(n_micro, flip_acts)
    loop(n_micro, backward)

    @at_last
    def _():
        loop(n_micro, flip_acts)

    def sums(m):
        for j in range(3):
            add_vec(2 + j, col_sum(dqkv[m, :, j * width:(j + 1) * width]))
        add_vec(5, col_sum(dres[m]))
        add_vec(8, col_sum(gbuf[m]))
        for j in range(n_tile):
            add_vec(9 + j, col_sum(dz[m, :, j * width:(j + 1) * width]))
    loop(n_micro, sums)

    vec_loc = pltpu.make_async_copy(vsum, vec_out.at[0], vec_sem.at[0])
    vec_far = remote(vsum, vec_out.at[1], vec_sem.at[1], vec_sem.at[2], device_id={'dp': mate})
    vec_loc.start()
    vec_far.start()
    for m in range(n_micro):
        before_last(fwd_copy(m).wait_send)
        past_first(bwd_copy(m).wait_send)
        for c in out_copies(m):
            c.wait()
        for loc, far in (fwd_exports(m), bwd_exports(m)):
            for c in loc + far:
                c.wait()
    vec_loc.wait()
    vec_far.wait()


def staggered(n, phases):
    for i in range(n + len(phases) - 1):
        for d, phase in reversed(list(enumerate(phases))):
            if 0 <= i - d < n:
                phase(i - d)


WEIGHTS = ('fc1', 'fc2', 'qkv', 'proj')
FIRST_Y = {'vec': True, 'fc1': True, 'qkv': True, 'fc2': False, 'proj': False}
ROWS = {'vec': 256, 'fc1': 768, 'qkv': 768, 'fc2': 1536, 'proj': 768}
TILES = {'vec': 1, 'fc1': 12, 'qkv': 9, 'fc2': 6, 'proj': 3}
WIDEST = {'vec': 1, 'fc1': 2, 'qkv': 2, 'fc2': 1, 'proj': 2}
WAYS = (1, -1)


def make_pieces():
    pieces, total = [], {}
    for name, tiles in TILES.items():
        k = -(-tiles // WIDEST[name])
        col = 0
        for i in range(k):
            cols = (tiles // k + (i < tiles % k)) * LANES
            way = min(WAYS, key=lambda w: total.get((FIRST_Y[name], w), 0))
            total[FIRST_Y[name], way] = total.get((FIRST_Y[name], way), 0) + cols * ROWS[name]
            pieces.append((name, way, col, cols))
            col += cols
    return pieces


def ring_of(piece, ph, ny, nz):
    return ny if FIRST_Y[piece[0]] == (ph == 1) else nz


def chain(piece, ph, typ, way, ny, nz):
    half = ring_of(piece, ph, ny, nz) // 2
    return half if (way == piece[1]) == (typ == 'rs') else half - 1


def make_order(pieces, ny, nz, rate=55.6e3, lat=3.434, first=3.0, ready=11.5, step=0.0626, weights=(1.678, 0.4223, -0.1187, 0.1025, 0.5053)):
    heap, order, waiting, free, done, ids = [], [], {}, {}, {}, iter(range(10**6))

    def nbytes(i, ph):
        rows = ROWS[pieces[i][0]] // ring_of(pieces[i], 1, ny, nz)
        return (rows if ph == 1 else rows // ring_of(pieces[i], 2, ny, nz)) * pieces[i][3] * 4

    def push(t, item):
        heapq.heappush(heap, (t, next(ids), item))

    def dispatch(t, key):
        queue = waiting.get(key)
        if queue and free.get(key, 0.0) <= t + 1e-9:
            ev = heapq.heappop(queue)[-1]
            w = nbytes(ev[1], ev[2]) / rate
            free[key] = t + w
            order.append(('send',) + ev)
            push(t + w, ('free', key))
            push(t + w + lat, ('land', ev))

    def enqueue(t, *ev):
        typ, i, ph, way, k = ev
        key = (FIRST_Y[pieces[i][0]] == (ph == 1), way)
        rank = (ph == 1, typ == 'ag', ph == 1 and typ == 'ag', k, i / len(pieces))
        rank = sum(a * b for a, b in zip(weights, rank))
        heapq.heappush(waiting.setdefault(key, []), (rank, next(ids), ev))
        dispatch(t, key)

    def start(t, typ, i, ph):
        for way in WAYS:
            if chain(pieces[i], ph, typ, way, ny, nz):
                enqueue(t, typ, i, ph, way, 0)

    for i in range(len(pieces)):
        push(first, ('start', i))
    seq = ready
    while heap:
        t, _, item = heapq.heappop(heap)
        if item[0] == 'free':
            dispatch(t, item[1])
        elif item[0] == 'start':
            start(t, 'rs', item[1], 1)
        elif item[0] == 'land':
            seq = max(seq, t) + step
            push(seq, ('done', item[1]))
        else:
            typ, i, ph, way, k = item[1]
            order.append(('recv',) + item[1])
            if k < chain(pieces[i], ph, typ, way, ny, nz) - 1:
                enqueue(t, typ, i, ph, way, k + 1)
            done[typ, i, ph] = done.get((typ, i, ph), 0) + 1
            if done[typ, i, ph] == ring_of(pieces[i], ph, ny, nz) - 1:
                if typ == 'rs':
                    start(t, 'rs' if ph == 1 else 'ag', i, 2)
                elif ph == 2:
                    start(t, 'ag', i, 1)
    return order


def grad_kernel(cfg, *refs):
    ny, nz, n_img, pieces, order = cfg
    n_p = len(pieces)
    it = iter(refs)
    take = lambda n: [next(it) for _ in range(n)]
    names = WEIGHTS
    each = lambda: dict(zip(names, take(len(names))))
    x_in, y_in = each(), each()
    vec_in = next(it)
    acc = each()
    acc['vec'] = next(it)
    mated = each()
    x_t, y_v = each(), each()
    vec_v = next(it)
    slots = {(i, ph, way): next(it) for ph in (1, 2) for way in WAYS for i in range(n_p)}
    ld_sem, send_sem, recv_sem, mate_send, mate_recv = take(5)

    dp = lax.axis_index('dp')
    core = lax.rem(dp, 2)
    mate = dp + 1 - 2 * core
    py = lax.rem(lax.div(dp, 2), ny)
    pz = lax.div(dp, 2 * ny)

    def at(y, z):
        return (z * ny + y) * 2 + core

    def turn(pos, by, n):
        return lax.rem(pos + by % n, n)

    nbr = {(True, 1): at(turn(py, 1, ny), pz), (True, -1): at(turn(py, -1, ny), pz),
           (False, 1): at(py, turn(pz, 1, nz)), (False, -1): at(py, turn(pz, -1, nz))}

    loads = []
    for j, name in enumerate(names):
        for s in range(n_img):
            loads.append((name, pltpu.make_async_copy(x_in[name].at[s], x_t[name].at[s], ld_sem.at[j, 0, s])))
            loads.append((name, pltpu.make_async_copy(y_in[name].at[s], y_v[name].at[s], ld_sem.at[j, 1, s])))
    vec_load = pltpu.make_async_copy(vec_in, vec_v, ld_sem.at[4, 0, 0])
    for _, ld in loads:
        ld.start()
    vec_load.start()

    barrier = pltpu.get_barrier_semaphore()
    for dev in list(nbr.values()) + [mate]:
        pl.semaphore_signal(barrier, device_id={'dp': dev}, device_id_type=MESH)

    pl.semaphore_wait(barrier, 5)

    def ring(i, ph):
        return ring_of(pieces[i], ph, ny, nz)

    def hops(i, ph, typ, way):
        return chain(pieces[i], ph, typ, way, ny, nz)

    def place(i, ph):
        return py if FIRST_Y[pieces[i][0]] == (ph == 1) else pz

    def rows_of(i, ph, by):
        size = ROWS[pieces[i][0]] // ring(i, 1)
        if ph == 1:
            start = turn(place(i, 1), by, ring(i, 1)) * size
        else:
            start, size = place(i, 1) * size, size // ring(i, 2)
            start = start + turn(place(i, 2), by, ring(i, 2)) * size
        return pl.ds(pl.multiple_of(start, 8), size)

    def view(i, ph, by):
        name, _, col, cols = pieces[i]
        return acc[name].at[rows_of(i, ph, by), col:col + cols]

    receives = {ev: j for j, ev in enumerate(o[1:] for o in order if o[0] == 'recv')}
    groups = {key: j for j, key in enumerate((typ, ph, way, i) for typ in ('rs', 'ag') for ph in (1, 2) for way in WAYS
                                             for i in range(n_p))}

    def landing(i, ph, way, k):
        n = hops(i, ph, 'ag', way)
        return slots[i, ph, -way].at[n - 2 - k if k <= n - 2 else n]

    def sent(typ, i, ph):
        for way in WAYS:
            n = hops(i, ph, typ, way)
            if n:
                part = slots[i, ph, way if typ == 'rs' else -way].at[:n]
                pltpu.make_async_copy(part, part, send_sem.at[groups[typ, ph, way, i]]).wait()

    def copy(typ, i, ph, way, k):
        if typ == 'rs':
            src, dst = view(i, ph, way * (hops(i, ph, typ, way) - k)), slots[i, ph, way].at[k]
        else:
            src = landing(i, ph, way, k - 1) if k else view(i, ph, 0)
            dst = landing(i, ph, way, k)
        dev = nbr[FIRST_Y[pieces[i][0]] == (ph == 1), way]
        return pltpu.make_async_remote_copy(src, dst, send_sem.at[groups[typ, ph, way, i]], recv_sem.at[receives[typ, i, ph, way, k]],
                                            device_id={'dp': dev}, device_id_type=MESH)

    def deliver(i, src, by):
        name, _, col, cols = pieces[i]
        if name != 'vec':
            pltpu.make_async_remote_copy(src, mated[name].at[rows_of(i, 1, by), col:col + cols], mate_send.at[i], mate_recv.at[i],
                                         device_id={'dp': mate}, device_id_type=MESH).start()

    lead = {name: next(j for j in range(n_p) if pieces[j][0] == name) for name in WEIGHTS}

    def multiply(t, name):
        i = lead[name]
        n = ring(i, 1)
        size = ROWS[name] // n
        by = (n // 2 - lax.div(t + 1, 2)) * (2 * lax.rem(t, 2) - 1)
        rows = pl.ds(pl.multiple_of(lax.rem(place(i, 1) + by + n, n) * size, 8), size)
        acc[name][rows, :] = sum(dot_nn(x_t[name][s, rows, :TOK], y_v[name][s]) for s in range(n_img))

    n_first = next(j for j, o in enumerate(order) if o[0] == 'recv')
    begin, todo = order[:n_first], order[n_first:]
    early = 3

    def send_early(name, t):
        for _, typ, i, ph, way, k in begin:
            far = hops(i, ph, typ, way) == ring(i, ph) // 2
            if pieces[i][0] == name and t == (0 if far else WAYS.index(way) + 1):
                copy(typ, i, ph, way, k).start()

    vec_load.wait()
    acc['vec'][...] = vec_v[0] + vec_v[1]
    for t in range(early):
        send_early('vec', t)

    def compute_early(t):
        for name in names:
            @pl.when(t == 0)
            def _():
                for nm, ld in loads:
                    if nm == name:
                        ld.wait()
            multiply(t, name)
            for j in range(early):
                pl.when(t == j)(functools.partial(send_early, name, j))
    loop(early, compute_early)
    for name in names:
        loop(ring(lead[name], 1) - early, lambda k, name=name: multiply(k + early, name))

    got = {}
    for what, *ev in todo:
        if what == 'send':
            copy(*ev).start()
            continue
        typ, i, ph, way, k = ev
        copy(*ev).wait_recv()
        got[typ, i, ph] = got.get((typ, i, ph), 0) + 1
        if typ == 'rs':
            dst = view(i, ph, way * (hops(i, ph, typ, way) - 1 - k))
            dst[...] = dst[...] + slots[i, ph, way][k]
        elif ph == 1:
            slot = landing(i, 1, way, k)
            deliver(i, slot, -way * (1 + k))
            if got[typ, i, ph] == 1:
                sent('rs', i, 1)
            dst = view(i, 1, -way * (1 + k))
            dst[...] = slot[...]
        elif got[typ, i, ph] == ring(i, 2) - 1:
            sent('rs', i, 2)
            for w in WAYS:
                for j in range(hops(i, 2, 'ag', w)):
                    dst = view(i, 2, -w * (1 + j))
                    dst[...] = landing(i, 2, w, j)[...]
            deliver(i, view(i, 1, 0), 0)

    for i in range(n_p):
        name, _, col, cols = pieces[i]
        for ph in (1, 2):
            sent('ag', i, ph)
        if name != 'vec':
            whole = acc[name].at[:, col:col + cols]
            pltpu.make_async_copy(whole, whole, mate_send.at[i]).wait()
            pltpu.make_async_copy(whole, whole, mate_recv.at[i]).wait()


def output_kernel(parts, *refs):
    it = iter(refs)
    take = lambda n: [next(it) for _ in range(n)]
    names = WEIGHTS
    n = len(names)
    own, vec, mated, acts = take(n), next(it), take(n), take(2)
    out, g_vec, g_b, joined = take(n), next(it), next(it), take(2)
    act_v, join_v, sem, act_sem = take(2), take(2), *take(2)
    core = lax.rem(lax.axis_index('dp'), 2)
    copies = []
    for j, name in enumerate(names):
        for c, src in ((core, own[j]), (1 - core, mated[j])):
            rows, cols = src.shape
            step = rows // parts[name]
            for r in range(0, rows, step):
                if name == 'fc2':
                    dst = out[j].at[pl.ds(pl.multiple_of(c * rows + r, 8), step), :]
                else:
                    dst = out[j].at[r:r + step, aligned(c * cols, cols)]
                copies.append(pltpu.make_async_copy(src.at[r:r + step], dst, sem.at[len(copies)]))
    reads = [pltpu.make_async_copy(acts[k], act_v[k], act_sem.at[k]) for k in range(2)]
    writes = [pltpu.make_async_copy(join_v[k], joined[k], act_sem.at[2 + k]) for k in range(2)]
    for c in reads + copies:
        c.start()
    n_vec, _, width = g_vec.shape
    per = width // LANES
    for i in range(n_vec):
        for t in range(per):
            g_vec[i, :, t * LANES:(t + 1) * LANES] = vec[i * per + t:i * per + t + 1, :]
    for t in range(g_b.shape[1] // LANES):
        g_b[:, t * LANES:(t + 1) * LANES] = vec[n_vec * per + t:n_vec * per + t + 1, :]
    for k in range(2):
        reads[k].wait()
        for m in range(join_v[k].shape[1]):
            join_v[k][:, m, :] = act_v[k][m, 0:join_v[k].shape[0]]
        writes[k].start()
    for c in copies + writes:
        c.wait()


def solution(mesh):
    stages = mesh.shape['pp']
    n_dp = mesh.shape['dp']
    ny = 4 if n_dp == 64 else 2
    nz = n_dp // (2 * ny)
    act_spec = P(None, 'dp')
    stage_spec = P('pp')
    out_act_spec = P('pp', None, 'dp')
    pieces = make_pieces()
    order = make_order(pieces, ny, nz)

    def per_device(x_in, grad_out, vectors, w_qkv, w_proj, w_fc1, b_fc1, w_fc2):
        n_micro, _, seq, width = x_in.shape
        mlp = w_fc1.shape[2]
        heads = w_proj.shape[1]
        x_p = x_in.reshape(n_micro, seq, width).transpose(1, 0, 2)
        go_p = grad_out.reshape(n_micro, seq, width).transpose(1, 0, 2)
        hbm, vmem = pl.BlockSpec(memory_space=pl.ANY), pl.BlockSpec(memory_space=pltpu.VMEM)
        n_img = 2 * n_micro
        act = lambda n, w: jax.ShapeDtypeStruct((n, TOK, w), BF16)
        flat = lambda f: jax.ShapeDtypeStruct((n_img, f, KEYS), BF16)
        dma, vm = pltpu.SemaphoreType.DMA, pltpu.VMEM
        outs = pl.pallas_call(
            functools.partial(pipeline_kernel, (seq, stages, n_micro)),
            name='pipeline',
            out_shape=[act(n_micro, width), act(n_micro, width), flat(width), flat(width), flat(width), flat(mlp // 2),
                       act(n_img, 3 * width // 2), act(n_img, mlp // 2), act(n_img, width // 2),
                       act(n_img, width), jax.ShapeDtypeStruct((2, 256, LANES), F32)],
            in_specs=[hbm, hbm, vmem, vmem, hbm, hbm, hbm, hbm],
            out_specs=[hbm] * 11,
            scratch_shapes=[
                vm((width, 3 * width), BF16), vm((width, width), BF16), vm((width, mlp), BF16), vm((mlp, width), BF16),
                vm((3 * width, width), BF16), vm((width, width), BF16), vm((mlp, width), BF16), vm((width, mlp), BF16),
                vm((n_micro, 3 * width + mlp, KEYS), BF16),
                vm((seq, n_micro, width), BF16), vm((seq, n_micro, width), BF16),
                vm((n_micro, TOK, width), BF16), vm((n_micro, TOK, width), BF16), vm((n_micro, TOK, width), BF16),
                vm((n_micro, TOK, width), BF16), vm((n_micro, TOK, width), BF16), vm((n_micro, KEYS, 3 * width), BF16),
                vm((n_micro, TOK, width), BF16), vm((n_micro, TOK, width), BF16), vm((n_micro, TOK, width), BF16),
                vm((n_micro, TOK, mlp), BF16), vm((n_micro, TOK, mlp), BF16), vm((n_micro, heads, TOK, KEYS), F32),
                vm((n_micro, heads, TOK, KEYS), BF16),
                vm((n_micro, 4, TOK, 1), F32), vm((n_micro, TOK, mlp), BF16), vm((n_micro, TOK, width), BF16),
                vm((KEYS, width), BF16), vm((TOK, width), BF16), vm((n_micro, TOK, 3 * width), BF16),
                vm((2, 2, TOK, KEYS), BF16), vm((2, 2, TOK, KEYS), BF16), vm((KEYS, LANES), F32),
                dma((4,)), dma((2,)), dma((2 * n_micro,)), dma((2 * n_micro,)), dma((n_micro, 10)),
                dma((n_micro, 8)), dma((n_micro, 8)), dma((3,)),
            ],
            compiler_params=pltpu.CompilerParams(collective_id=0, has_side_effects=True, vmem_limit_bytes=67043328),
        )(x_p, go_p, vectors[0], b_fc1, w_qkv[0], w_proj[0].reshape(width, width), w_fc1[0], w_fc2[0])
        so, sg, xa1, xa2, xo, xf, dqkv, dz, dr, gy, vec = outs

        half = {'fc1': mlp // 2, 'fc2': width, 'qkv': 3 * width // 2, 'proj': width // 2}
        feats = {'fc1': width, 'fc2': mlp // 2, 'qkv': width, 'proj': width}
        names = WEIGHTS
        f32 = lambda *s: jax.ShapeDtypeStruct(s, F32)
        slots = []
        for ph in (1, 2):
            for way in WAYS:
                for piece in pieces:
                    rows = ROWS[piece[0]] // ring_of(piece, 1, ny, nz)
                    rows = rows if ph == 1 else rows // ring_of(piece, 2, ny, nz)
                    slots.append(vm((chain(piece, ph, 'rs', way, ny, nz) + 1, rows, piece[3]), F32))
        n_recv = len([o for o in order if o[0] == 'recv'])
        grads = pl.pallas_call(
            functools.partial(grad_kernel, (ny, nz, n_img, pieces, order)),
            name='gradients',
            out_shape=[vm((feats[n], half[n]), F32) for n in names] + [vm((256, LANES), F32)]
            + [vm((feats[n], half[n]), F32) for n in names],
            in_specs=[hbm] * 9,
            out_specs=[vmem] * 9,
            scratch_shapes=(
                [vm((n_img, feats[n], KEYS), BF16) for n in names] + [vm((n_img, TOK, half[n]), BF16) for n in names]
                + [vm((2, 256, LANES), F32)] + slots
                + [dma((5, 2, n_img)), dma((8 * len(pieces),)), dma((n_recv,)), dma((len(pieces),)), dma((len(pieces),))]),
            compiler_params=pltpu.CompilerParams(collective_id=1, has_side_effects=True, vmem_limit_bytes=37 * 10**6),
        )(xa2, xf, xa1, xo, dz, gy, dqkv, dr, vec)
        parts = {'fc1': 3, 'fc2': 3, 'qkv': 3, 'proj': 1}
        raw = jax.ShapeDtypeStruct((seq, n_micro, width), BF16)
        g_fc1, g_fc2, g_qkv, g_proj, g_vectors, g_bfc1, so, sg = pl.pallas_call(
            functools.partial(output_kernel, parts),
            name='outputs',
            out_shape=[f32(width, mlp), f32(mlp, width), f32(width, 3 * width), f32(width, width), f32(vectors.shape[1], 1, width),
                       f32(1, mlp), raw, raw],
            in_specs=[vmem] * 9 + [hbm] * 2,
            out_specs=[hbm] * 4 + [vmem] * 2 + [hbm] * 2,
            scratch_shapes=[vm((n_micro, TOK, width), BF16)] * 2 + [vm((seq, n_micro, width), BF16)] * 2
            + [dma((2 * sum(parts.values()),)), dma((4,))],
            compiler_params=pltpu.CompilerParams(vmem_limit_bytes=5 * 1024 * 1024),
        )(*grads, so, sg)
        so, sg = [t.transpose(1, 0, 2).reshape(1, n_micro, 1, seq, width) for t in (so, sg)]
        return (so, sg, g_vectors.transpose(1, 0, 2), g_qkv[None], g_proj.reshape(1, heads, width // heads, width), g_fc1[None], g_bfc1,
                g_fc2[None])

    return jax.shard_map(per_device, mesh=mesh, in_specs=(act_spec, act_spec) + (stage_spec,) * 6,
                         out_specs=(out_act_spec, out_act_spec) + (stage_spec,) * 6, check_vma=False)
```
